512 devices in a mesh: row: 32 (over y, z_lo), col: 16 (over z_hi, x, core).
Axes of the slice: x: 4, y: 4, z: 16 (z_hi: 2, z_lo: 8; z = z_hi * 8 + z_lo), core: 2. Of those that a mesh axis runs over, the one named last changes fastest.
Arguments:
- embeddings: bfloat16 [5, 192, 32768], P(None, None, ('row', 'col')), may hold values from -6 to 6
- scale_weights: float32 [5], replicated, may hold values from 0.1 to 0.5
- vectors: bfloat16 [32, 32768], P(None, ('row', 'col')), may hold values from -6 to 6
Outputs:
- product: float32 [32, 32768], P(None, ('row', 'col'))
The draws below stay inside these ranges and needn't reach their ends.
All inputs are finite; a program needn't handle non-finite values.
Results may differ from the reference program's by a relative error of at most 0.011.
Values may be sent and summed in bfloat16 or wider, within the bound.
No kernel may reach another device: no remote copies, remote signals or barrier semaphores. Data moves between devices by JAX's collectives and lax.ppermute only.
A program may use at most 64 MiB of HBM per device.

```python
import math
import jax
import jax.numpy as jnp
from jax import lax

DIM = 192
SCALES = 5
VECS = 32
SEGMENTS = 32768


def block_scale(stream_key, extent, cuts, least, top_value):
    loudness, own = 1.0, jax.random.fold_in(stream_key, 6)
    for position, parts in cuts:
        heights = jnp.exp(jax.random.uniform(jax.random.fold_in(own, position), (parts,), jnp.float32, least / len(cuts), top_value / len(cuts)))
        loudness = loudness * jnp.repeat(heights, extent[position] // parts).reshape([-1 if axis == position else 1 for axis in range(len(extent))])
    return loudness


def bell_draw(stream_key, extent, width, bound, split=(), kind=jnp.bfloat16):
    values = jax.random.normal(stream_key, extent, jnp.float32) * width
    if len(split) > 0:
        values = block_scale(stream_key, extent, split, -0.22, 0.18) * values
    return jnp.clip(values, min=-bound, max=bound).astype(kind)


def setup_inputs(seed: int = 0) -> dict:
    arg_keys = jax.random.split(jax.random.key(seed), 4)
    return {
        "embeddings": bell_draw(arg_keys[0], (SCALES, DIM, SEGMENTS), 1.0, 6.0, ((2, 512),)),
        "scale_weights": jnp.clip(jnp.exp(jax.random.uniform(arg_keys[1], (SCALES,), jnp.float32, math.log(0.1), math.log(0.5))), 0.1, 0.5),
        "vectors": bell_draw(arg_keys[2], (VECS, SEGMENTS), 1.0, 6.0, ((1, 512),)),
    }


SHARP = 3.5

def reference(embeddings, scale_weights, vectors):
    total = embeddings.shape[2]
    values = embeddings.astype(jnp.float32)
    units = values * lax.rsqrt(lax.optimization_barrier(jnp.sum(values * values, axis=1, keepdims=True)) + 1e-06)
    unit = lax.optimization_barrier(units.astype(jnp.bfloat16))
    weighted = (scale_weights[:, None, None] * unit.astype(jnp.float32)).astype(jnp.bfloat16)
    row_panel = weighted.reshape(-1, total)
    column_panel = unit.reshape(-1, total)
    sharpness = SHARP * math.sqrt(DIM)
    stride = math.gcd(total, 512)
    columns = jnp.arange(total, dtype=jnp.int32)

    def one_block(offset):
        rows = lax.dynamic_slice_in_dim(row_panel, offset, stride, 1)
        cosine = lax.dot_general(rows, column_panel, (((0,), (0,)), ((), ())), preferred_element_type=jnp.float32)
        row_ids = offset + jnp.arange(stride, dtype=jnp.int32)
        affinity = jnp.where(row_ids[:, None] == columns[None, :], jnp.zeros_like(cosine), jnp.exp(sharpness * cosine))
        degree = lax.optimization_barrier(jnp.sum(affinity, axis=1))
        numerator = lax.dot_general(vectors, affinity.astype(jnp.bfloat16), (((1,), (1,)), ((), ())), preferred_element_type=jnp.float32)
        return numerator / degree[None, :]
    offsets = jnp.arange(total // stride, dtype=jnp.int32) * stride
    blocks = lax.map(one_block, offsets)
    return jnp.transpose(blocks, (1, 0, 2)).reshape(vectors.shape[0], total)
```

```python
import math

import jax
import jax.numpy as jnp
from jax import lax
from jax.experimental import pallas as pl
from jax.experimental.pallas import tpu as pltpu
from jax.sharding import Mesh
from jax.sharding import PartitionSpec as P

SHARP = 3.5
AXES = ("y", "zl", "zh", "x", "core")
PLANE = ("y", "x")
LINE = ("zh", "zl", "core")
LANES = 1024
TILE = 256
VMEM = pl.BlockSpec(memory_space=pltpu.VMEM)
SMEM = pl.BlockSpec(memory_space=pltpu.SMEM)


def grant(mib):
    return pltpu.CompilerParams(vmem_limit_bytes=mib << 20)


def prepare_kernel(weights_ref, embeddings_ref, vectors_ref, rows_ref, item_ref):
    scales, segments, dim = embeddings_ref.shape
    vecs = vectors_ref.shape[0]
    units, weighted = [], []
    for scale in range(scales):
        values = embeddings_ref[scale].astype(jnp.float32)
        norm = jnp.sum(values * values, axis=1, keepdims=True) + 1e-06
        unit = (values * lax.rsqrt(norm)).astype(jnp.bfloat16).astype(jnp.float32)
        units.append(unit)
        weighted.append(weights_ref[scale] * unit)
    vectors = vectors_ref[...].astype(jnp.float32)
    top = jnp.max(jnp.abs(vectors), axis=1, keepdims=True)
    power = jnp.ceil(jnp.log2(jnp.maximum(top, 2.0**-120)))
    scaled = vectors * jnp.exp2(-power)
    powers = jnp.broadcast_to(power, (vecs, segments))
    extra = jnp.concatenate([scaled, powers], axis=0).T
    rest = LANES - scales * dim
    zeros = jnp.zeros((segments, rest), jnp.float32)
    row_item = jnp.concatenate(weighted + [zeros], axis=1).astype(jnp.bfloat16)
    for peer in range(rows_ref.shape[0]):
        rows_ref[peer] = row_item
    tail = [jnp.zeros((segments, rest - 2 * vecs), jnp.float32)] if rest > 2 * vecs else []
    item_ref[...] = jnp.concatenate(units + [extra] + tail, axis=1)


def tile_kernel(depth, vecs, sharpness, starts_ref, rows_ref, columns_ref, out_ref):
    row_start, column_start = starts_ref[0], starts_ref[1]
    segments = starts_ref[2]
    row_count, column_count = rows_ref.shape[0], columns_ref.shape[0]
    row_place = lax.broadcasted_iota(jnp.int32, (row_count, 1), 0) - row_start
    row_place = jnp.where((row_place >= 0) & (row_place < segments), row_place, -1)
    total = jnp.zeros((row_count, 128), jnp.float32)
    for start in range(0, column_count, TILE):
        columns = columns_ref[start : start + TILE, :]
        cosine = lax.dot_general(
            rows_ref[...], columns, (((1,), (1,)), ((), ())), preferred_element_type=jnp.float32
        )
        place = lax.broadcasted_iota(jnp.int32, (1, TILE), 1) + (start - column_start)
        place = jnp.where((place >= 0) & (place < segments), place, -2)
        affinity = jnp.where(row_place == place, 0.0, jnp.exp2(cosine * sharpness))
        tail = columns[:, depth:].astype(jnp.float32)
        vectors = tail[:, :vecs] * jnp.exp2(tail[:, vecs : 2 * vecs])
        ones = jnp.ones((TILE, 1), jnp.float32)
        blank = jnp.zeros((TILE, 127 - vecs), jnp.float32)
        right = jnp.concatenate([vectors, ones, blank], axis=1).astype(jnp.bfloat16)
        total += jnp.dot(
            affinity.astype(jnp.bfloat16), right, preferred_element_type=jnp.float32
        )
    out_ref[...] = total.reshape(out_ref.shape)


def finish_kernel(parts_ref, out_ref):
    vecs = out_ref.shape[0]
    total = jnp.sum(parts_ref[...], axis=0).T
    out_ref[...] = total[:vecs] / total[vecs : vecs + 1]


def shards(embeddings, scale_weights, vectors):
    scales, dim, segments = embeddings.shape
    vecs = vectors.shape[0]
    peers = lax.axis_size(PLANE)
    line = lax.axis_size(LINE)
    sharpness = SHARP * math.sqrt(dim) * math.log2(math.e)
    row_copies, item = pl.pallas_call(
        prepare_kernel,
        out_shape=(
            jax.ShapeDtypeStruct((peers, segments, LANES), jnp.bfloat16),
            jax.ShapeDtypeStruct((segments, LANES), jnp.float32),
        ),
        in_specs=[SMEM, VMEM, VMEM],
        out_specs=(VMEM, VMEM),
        compiler_params=grant(4),
        name="prepare",
    )(scale_weights, jnp.swapaxes(embeddings, 1, 2), vectors)
    rows = lax.all_to_all(row_copies, PLANE, 0, 0, tiled=True)
    columns = lax.all_gather(item.astype(jnp.float16), LINE, axis=0, tiled=True)
    columns = columns.astype(jnp.bfloat16)
    starts = jnp.stack(
        [
            lax.axis_index(PLANE) * segments,
            lax.axis_index(LINE) * segments,
            jnp.int32(segments),
        ]
    )
    sums = pl.pallas_call(
        lambda *refs: tile_kernel(scales * dim, vecs, sharpness, *refs),
        out_shape=jax.ShapeDtypeStruct((peers, segments, 128), jnp.float32),
        in_specs=[SMEM, VMEM, VMEM],
        out_specs=VMEM,
        compiler_params=grant(16),
        name="tile",
    )(starts, rows.reshape(peers * segments, LANES), columns)
    parts = lax.all_to_all(sums, PLANE, 0, 0, tiled=True)
    return pl.pallas_call(
        finish_kernel,
        out_shape=jax.ShapeDtypeStruct((vecs, segments), jnp.float32),
        in_specs=[VMEM],
        out_specs=VMEM,
        compiler_params=grant(2),
        name="finish",
    )(parts)


def solution(mesh):
    torus = Mesh(mesh.devices.reshape(4, 8, 2, 4, 2), AXES)
    return jax.shard_map(
        shards,
        mesh=torus,
        in_specs=(P(None, None, AXES), P(), P(None, AXES)),
        out_specs=P(None, AXES),
        check_vma=False,
    )
```

```python
import math

import jax
import jax.numpy as jnp
from jax import lax
from jax.experimental import pallas as pl
from jax.experimental.pallas import tpu as pltpu
from jax.sharding import Mesh
from jax.sharding import PartitionSpec as P

SHARP = 3.5
AXES = ("y", "zl", "zh", "x", "core")
PLANE = ("y", "x")
LINE = ("zh", "zl", "core")
LANES = 1024
TILE = 256
STRIP = 256
VMEM = pl.BlockSpec(memory_space=pltpu.VMEM)
HBM = pl.BlockSpec(memory_space=pltpu.HBM)
SMEM = pl.BlockSpec(memory_space=pltpu.SMEM)


def grant(mib):
    return pltpu.CompilerParams(vmem_limit_bytes=mib << 20)


def prepare_kernel(
    weights_hbm, embeddings_hbm, vectors_hbm, rows_hbm, item_ref,
    weights_ref, embeddings_ref, vectors_ref, row_ref, in_sems, out_sems
):
    loads = [
        pltpu.make_async_copy(source, target, in_sems.at[place])
        for place, (source, target) in enumerate(
            [
                (weights_hbm, weights_ref),
                (embeddings_hbm, embeddings_ref),
                (vectors_hbm, vectors_ref),
            ]
        )
    ]
    for load in loads:
        load.start()
    for load in loads:
        load.wait()
    scales, segments, dim = embeddings_ref.shape
    vecs = vectors_ref.shape[0]
    units, weighted = [], []
    for scale in range(scales):
        values = embeddings_ref[scale].astype(jnp.float32)
        norm = jnp.sum(values * values, axis=1, keepdims=True) + 1e-06
        unit = (values * lax.rsqrt(norm)).astype(jnp.bfloat16).astype(jnp.float32)
        units.append(unit)
        weighted.append(weights_ref[0, scale] * unit)
    rest = LANES - scales * dim
    zeros = jnp.zeros((segments, rest), jnp.float32)
    row_ref[...] = jnp.concatenate(weighted + [zeros], axis=1).astype(jnp.bfloat16)
    stores = [
        pltpu.make_async_copy(row_ref, rows_hbm.at[peer], out_sems.at[peer])
        for peer in range(rows_hbm.shape[0])
    ]
    for store in stores:
        store.start()
    vectors = vectors_ref[...].astype(jnp.float32)
    top = jnp.max(jnp.abs(vectors), axis=1, keepdims=True)
    power = jnp.ceil(jnp.log2(jnp.maximum(top, 2.0**-120)))
    scaled = vectors * jnp.exp2(-power)
    powers = jnp.broadcast_to(power, (vecs, segments))
    extra = jnp.concatenate([scaled, powers], axis=0).T
    tail = [jnp.zeros((segments, rest - 2 * vecs), jnp.float32)] if rest > 2 * vecs else []
    item_ref[...] = jnp.concatenate(units + [extra] + tail, axis=1)
    for store in stores:
        store.wait()


def tile_kernel(depth, vecs, sharpness, starts_ref, rows_ref, columns_ref, out_ref):
    row_count, column_count = rows_ref.shape[0], columns_ref.shape[0]
    row_start, column_start, segments = starts_ref[0], starts_ref[1], starts_ref[2]
    width = out_ref.shape[2] // 2
    row_place = lax.broadcasted_iota(jnp.int32, (row_count, 1), 0) - row_start
    row_place = jnp.where((row_place >= 0) & (row_place < segments), row_place, -1)
    totals = [jnp.zeros((STRIP, 128), jnp.float32) for _ in range(row_count // STRIP)]
    for start in range(0, column_count, TILE):
        place = lax.broadcasted_iota(jnp.int32, (1, TILE), 1) + (start - column_start)
        place = jnp.where((place >= 0) & (place < segments), place, -2)
        columns = columns_ref[start : start + TILE, :]
        tail = columns[:, depth:].astype(jnp.float32)
        vectors = tail[:, :vecs] * jnp.exp2(tail[:, vecs : 2 * vecs])
        ones = jnp.ones((TILE, 1), jnp.float32)
        blank = jnp.zeros((TILE, 127 - vecs), jnp.float32)
        right = jnp.concatenate([vectors, ones, blank], axis=1).astype(jnp.bfloat16)
        for strip in range(len(totals)):
            span = slice(strip * STRIP, (strip + 1) * STRIP)
            cosine = lax.dot_general(
                rows_ref[span, :],
                columns,
                (((1,), (1,)), ((), ())),
                preferred_element_type=jnp.float32,
            )
            affinity = jnp.where(row_place[span] == place, 0.0, jnp.exp2(cosine * sharpness))
            totals[strip] += jnp.dot(
                affinity.astype(jnp.bfloat16), right, preferred_element_type=jnp.float32
            )
    half = vecs // 2
    for strip, total in enumerate(totals):
        sums = total.T
        for peer in range(STRIP // width):
            part = sums[: vecs + 1, peer * width : (peer + 1) * width]
            place = strip * (STRIP // width) + peer
            out_ref[place, :half, :width] = part[:half]
            out_ref[place, :half, width:] = part[half:vecs]
            out_ref[place, half : half + 1, :width] = part[vecs:]
            out_ref[place, half : half + 1, width:] = part[vecs:]


def finish_kernel(parts_ref, out_ref):
    half, width = out_ref.shape[0] // 2, out_ref.shape[1]
    total = jnp.sum(parts_ref[...], axis=0)
    product = total[:half] / total[half : half + 1]
    out_ref[:half] = product[:, :width]
    out_ref[half:] = product[:, width:]


def shards(embeddings, scale_weights, vectors):
    scales, dim, segments = embeddings.shape
    vecs = vectors.shape[0]
    peers = lax.axis_size(PLANE)
    packed = vecs // 2 + 8
    sharpness = SHARP * math.sqrt(dim) * math.log2(math.e)
    row_copies, item = pl.pallas_call(
        prepare_kernel,
        out_shape=(
            jax.ShapeDtypeStruct((peers, segments, LANES), jnp.bfloat16),
            jax.ShapeDtypeStruct((segments, LANES), jnp.float32),
        ),
        in_specs=[HBM, HBM, HBM],
        out_specs=(HBM, VMEM),
        scratch_shapes=[
            pltpu.SMEM((1, scales), jnp.float32),
            pltpu.VMEM((scales, segments, dim), jnp.bfloat16),
            pltpu.VMEM((vecs, segments), jnp.bfloat16),
            pltpu.VMEM((segments, LANES), jnp.bfloat16),
            pltpu.SemaphoreType.DMA((3,)),
            pltpu.SemaphoreType.DMA((peers,)),
        ],
        compiler_params=grant(60),
        name="prepare",
    )(scale_weights[None], jnp.swapaxes(embeddings, 1, 2), vectors)
    rows = lax.all_to_all(row_copies, PLANE, 0, 0, tiled=True)
    columns = lax.all_gather(item.astype(jnp.float16), LINE, axis=0, tiled=True)
    columns = columns.astype(jnp.bfloat16)
    starts = jnp.stack(
        [
            lax.axis_index(PLANE) * segments,
            lax.axis_index(LINE) * segments,
            jnp.int32(segments),
        ]
    )
    row_count, column_count = peers * segments, columns.shape[0]
    sums = pl.pallas_call(
        lambda *refs: tile_kernel(scales * dim, vecs, sharpness, *refs),
        out_shape=jax.ShapeDtypeStruct((peers, packed, 2 * segments), jnp.float32),
        in_specs=[SMEM, VMEM, VMEM],
        out_specs=VMEM,
        compiler_params=grant(16),
        name="tile",
    )(starts, rows.reshape(row_count, LANES), columns)
    parts = lax.all_to_all(sums, PLANE, 0, 0, tiled=True)
    return pl.pallas_call(
        finish_kernel,
        out_shape=jax.ShapeDtypeStruct((vecs, segments), jnp.float32),
        in_specs=[VMEM],
        out_specs=VMEM,
        compiler_params=grant(2),
        name="finish",
    )(parts)


def solution(mesh):
    torus = Mesh(mesh.devices.reshape(4, 8, 2, 4, 2), AXES)
    return jax.shard_map(
        shards,
        mesh=torus,
        in_specs=(P(None, None, AXES), P(), P(None, AXES)),
        out_specs=P(None, AXES),
        check_vma=False,
    )
```

```python
import math

import jax
import jax.numpy as jnp
from jax import lax
from jax.experimental import pallas as pl
from jax.experimental.pallas import tpu as pltpu
from jax.sharding import Mesh
from jax.sharding import PartitionSpec as P

SHARP = 3.5
AXES = ("y", "zl", "zh", "x", "core")
PLANE = ("y", "x")
LINE = ("zh", "zl", "core")
LANES = 1024
TILE = 512
VMEM = pl.BlockSpec(memory_space=pltpu.VMEM)
HBM = pl.BlockSpec(memory_space=pltpu.HBM)
SMEM = pl.BlockSpec(memory_space=pltpu.SMEM)


def grant(mib):
    return pltpu.CompilerParams(vmem_limit_bytes=mib << 20)


def prepare_kernel(
    weights_hbm, embeddings_hbm, vectors_hbm, rows_hbm, item_ref,
    weights_ref, embeddings_ref, vectors_ref, row_ref, in_sems, out_sems
):
    loads = [
        pltpu.make_async_copy(source, target, in_sems.at[place])
        for place, (source, target) in enumerate(
            [
                (weights_hbm, weights_ref),
                (embeddings_hbm, embeddings_ref),
                (vectors_hbm, vectors_ref),
            ]
        )
    ]
    for load in loads:
        load.start()
    for load in loads:
        load.wait()
    scales, segments, dim = embeddings_ref.shape
    vecs = vectors_ref.shape[0]
    units, weighted = [], []
    for scale in range(scales):
        values = embeddings_ref[scale].astype(jnp.float32)
        norm = jnp.sum(values * values, axis=1, keepdims=True) + 1e-06
        unit = (values * lax.rsqrt(norm)).astype(jnp.bfloat16).astype(jnp.float32)
        units.append(unit)
        weighted.append(weights_ref[0, scale] * unit)
    rest = LANES - scales * dim
    zeros = jnp.zeros((segments, rest), jnp.float32)
    row_ref[...] = jnp.concatenate(weighted + [zeros], axis=1).astype(jnp.bfloat16)
    stores = [
        pltpu.make_async_copy(row_ref, rows_hbm.at[peer], out_sems.at[peer])
        for peer in range(rows_hbm.shape[0])
    ]
    for store in stores:
        store.start()
    vectors = vectors_ref[...].astype(jnp.float32)
    top = jnp.max(jnp.abs(vectors), axis=1, keepdims=True)
    power = jnp.ceil(jnp.log2(jnp.maximum(top, 2.0**-120)))
    scaled = vectors * jnp.exp2(-power)
    powers = jnp.broadcast_to(power, (vecs, segments))
    extra = jnp.concatenate([scaled, powers], axis=0).T
    tail = [jnp.zeros((segments, rest - 2 * vecs), jnp.float32)] if rest > 2 * vecs else []
    item_ref[...] = jnp.concatenate(units + [extra] + tail, axis=1)
    for store in stores:
        store.wait()


def tile_kernel(depth, vecs, sharpness, starts_ref, rows_ref, columns_ref, out_ref):
    row_count, column_count = rows_ref.shape[0], columns_ref.shape[0]
    row_start, column_start, segments = starts_ref[0], starts_ref[1], starts_ref[2]
    width = out_ref.shape[2] // 2
    row_place = lax.broadcasted_iota(jnp.int32, (row_count, 1), 0) - row_start
    row_place = jnp.where((row_place >= 0) & (row_place < segments), row_place, -1)
    total = jnp.zeros((row_count, 128), jnp.float32)
    for start in range(0, column_count, TILE):
        place = lax.broadcasted_iota(jnp.int32, (1, TILE), 1) + (start - column_start)
        place = jnp.where((place >= 0) & (place < segments), place, -2)
        columns = columns_ref[start : start + TILE, :]
        tail = columns[:, depth:].astype(jnp.float32)
        vectors = tail[:, :vecs] * jnp.exp2(tail[:, vecs : 2 * vecs])
        ones = jnp.ones((TILE, 1), jnp.float32)
        blank = jnp.zeros((TILE, 127 - vecs), jnp.float32)
        right = jnp.concatenate([vectors, ones, blank], axis=1).astype(jnp.bfloat16)
        cosine = lax.dot_general(
            rows_ref[...], columns, (((1,), (1,)), ((), ())), preferred_element_type=jnp.float32
        )
        affinity = jnp.where(row_place == place, 0.0, jnp.exp2(cosine * sharpness))
        total += jnp.dot(
            affinity.astype(jnp.bfloat16), right, preferred_element_type=jnp.float32
        )
    half = vecs // 2
    sums = total.T
    for peer in range(out_ref.shape[0]):
        part = sums[: vecs + 1, peer * width : (peer + 1) * width]
        out_ref[peer, :half, :width] = part[:half]
        out_ref[peer, :half, width:] = part[half:vecs]
        out_ref[peer, half : half + 1, :width] = part[vecs:]
        out_ref[peer, half : half + 1, width:] = part[vecs:]


def finish_kernel(parts_ref, out_ref):
    half, width = out_ref.shape[0] // 2, out_ref.shape[1]
    total = jnp.sum(parts_ref[...], axis=0)
    product = total[:half] / total[half : half + 1]
    out_ref[:half] = product[:, :width]
    out_ref[half:] = product[:, width:]


def shards(embeddings, scale_weights, vectors):
    scales, dim, segments = embeddings.shape
    vecs = vectors.shape[0]
    peers = lax.axis_size(PLANE)
    packed = vecs // 2 + 8
    sharpness = SHARP * math.sqrt(dim) * math.log2(math.e)
    row_copies, item = pl.pallas_call(
        prepare_kernel,
        out_shape=(
            jax.ShapeDtypeStruct((peers, segments, LANES), jnp.bfloat16),
            jax.ShapeDtypeStruct((segments, LANES), jnp.float32),
        ),
        in_specs=[HBM, HBM, HBM],
        out_specs=(HBM, VMEM),
        scratch_shapes=[
            pltpu.SMEM((1, scales), jnp.float32),
            pltpu.VMEM((scales, segments, dim), jnp.bfloat16),
            pltpu.VMEM((vecs, segments), jnp.bfloat16),
            pltpu.VMEM((segments, LANES), jnp.bfloat16),
            pltpu.SemaphoreType.DMA((3,)),
            pltpu.SemaphoreType.DMA((peers,)),
        ],
        compiler_params=grant(60),
        name="prepare",
    )(scale_weights[None], jnp.swapaxes(embeddings, 1, 2), vectors)
    rows = lax.all_to_all(row_copies, PLANE, 0, 0, tiled=True)
    columns = lax.all_gather(item.astype(jnp.float16), LINE, axis=0, tiled=True)
    columns = columns.astype(jnp.bfloat16)
    starts = jnp.stack(
        [
            lax.axis_index(PLANE) * segments,
            lax.axis_index(LINE) * segments,
            jnp.int32(segments),
        ]
    )
    row_count, column_count = peers * segments, columns.shape[0]
    sums = pl.pallas_call(
        lambda *refs: tile_kernel(scales * dim, vecs, sharpness, *refs),
        out_shape=jax.ShapeDtypeStruct((peers, packed, 2 * segments), jnp.float32),
        in_specs=[SMEM, VMEM, VMEM],
        out_specs=VMEM,
        compiler_params=grant(24),
        name="tile",
    )(starts, rows.reshape(row_count, LANES), columns)
    parts = lax.all_to_all(sums, PLANE, 0, 0, tiled=True)
    return pl.pallas_call(
        finish_kernel,
        out_shape=jax.ShapeDtypeStruct((vecs, segments), jnp.float32),
        in_specs=[VMEM],
        out_specs=VMEM,
        compiler_params=grant(2),
        name="finish",
    )(parts)


def solution(mesh):
    torus = Mesh(mesh.devices.reshape(4, 8, 2, 4, 2), AXES)
    return jax.shard_map(
        shards,
        mesh=torus,
        in_specs=(P(None, None, AXES), P(), P(None, AXES)),
        out_specs=P(None, AXES),
        check_vma=False,
    )
```

```python
import math

import jax
import jax.numpy as jnp
from jax import lax
from jax.experimental import pallas as pl
from jax.experimental.pallas import tpu as pltpu
from jax.sharding import Mesh
from jax.sharding import PartitionSpec as P

SHARP = 3.5
AXES = ("y", "zl", "zh", "x", "core")
PLANE = ("y", "x")
LINE = ("zh", "zl", "core")
LANES = 1024
TILE = 512
FIRST = 256
PART = 32
VMEM = pl.BlockSpec(memory_space=pltpu.VMEM)
HBM = pl.BlockSpec(memory_space=pltpu.HBM)
SMEM = pl.BlockSpec(memory_space=pltpu.SMEM)


def grant(mib):
    return pltpu.CompilerParams(vmem_limit_bytes=mib << 20)


def prepare_kernel(
    weights_hbm, embeddings_hbm, vectors_hbm, rows_hbm, item_hbm,
    weights_ref, embeddings_ref, vectors_ref, row_ref, item_ref, in_sems, out_sems, item_sem
):
    scales, segments, dim = embeddings_ref.shape
    vecs, peers = vectors_ref.shape[0], rows_hbm.shape[0]
    count = segments // PART
    loads = [
        pltpu.make_async_copy(weights_hbm, weights_ref, in_sems.at[0]),
        pltpu.make_async_copy(vectors_hbm, vectors_ref, in_sems.at[1]),
    ] + [
        pltpu.make_async_copy(
            embeddings_hbm.at[:, part * PART : (part + 1) * PART],
            embeddings_ref.at[:, part * PART : (part + 1) * PART],
            in_sems.at[2 + part],
        )
        for part in range(count)
    ]
    for load in loads[2:] + loads[:2]:
        load.start()
    rest = LANES - scales * dim
    row_ref[:, scales * dim :] = jnp.zeros((segments, rest), jnp.bfloat16)
    loads[0].wait()
    stores = []
    for part in range(count):
        loads[2 + part].wait()
        span = slice(part * PART, (part + 1) * PART)
        units, weighted = [], []
        for scale in range(scales):
            values = embeddings_ref[scale, span, :].astype(jnp.float32)
            norm = jnp.sum(values * values, axis=1, keepdims=True) + 1e-06
            unit = (values * lax.rsqrt(norm)).astype(jnp.bfloat16).astype(jnp.float32)
            units.append(unit)
            weighted.append(weights_ref[0, scale] * unit)
        row_ref[span, : scales * dim] = jnp.concatenate(weighted, axis=1).astype(jnp.bfloat16)
        for peer in range(peers):
            store = pltpu.make_async_copy(
                row_ref.at[span], rows_hbm.at[peer, span], out_sems.at[part, peer]
            )
            store.start()
            stores.append(store)
        item_ref[span, : scales * dim] = jnp.concatenate(units, axis=1).astype(jnp.bfloat16)
    loads[1].wait()
    vectors = vectors_ref[...].astype(jnp.float32)
    top = jnp.max(jnp.abs(vectors), axis=1, keepdims=True)
    power = jnp.ceil(jnp.log2(jnp.maximum(top, 2.0**-120)))
    scaled = vectors * jnp.exp2(-power)
    powers = jnp.broadcast_to(power, (vecs, segments))
    extra = jnp.concatenate([scaled, powers], axis=0).T
    if rest > 2 * vecs:
        tail = jnp.zeros((segments, rest - 2 * vecs), jnp.float32)
        extra = jnp.concatenate([extra, tail], axis=1)
    item_ref[:, scales * dim :] = extra.astype(jnp.bfloat16)
    keep = pltpu.make_async_copy(item_ref, item_hbm, item_sem)
    keep.start()
    for store in stores:
        store.wait()
    keep.wait()


def tile_kernel(
    depth, vecs, sharpness, starts_ref, rows_ref, columns_hbm, out_ref, columns_ref, sems
):
    bounds = [0] + list(range(FIRST, columns_ref.shape[0], TILE)) + [columns_ref.shape[0]]
    spans = [slice(start, stop) for start, stop in zip(bounds[:-1], bounds[1:])]
    loads = [
        pltpu.make_async_copy(columns_hbm.at[span], columns_ref.at[span], sems.at[place])
        for place, span in enumerate(spans)
    ]
    for load in loads:
        load.start()
    row_count = rows_ref.shape[0]
    row_start, column_start, segments = starts_ref[0], starts_ref[1], starts_ref[2]
    width = out_ref.shape[2] // 2
    row_place = lax.broadcasted_iota(jnp.int32, (row_count, 1), 0) - row_start
    row_place = jnp.where((row_place >= 0) & (row_place < segments), row_place, -1)
    total = jnp.zeros((row_count, 128), jnp.float32)
    for span, load in zip(spans, loads):
        load.wait()
        size = span.stop - span.start
        place = lax.broadcasted_iota(jnp.int32, (1, size), 1) + (span.start - column_start)
        place = jnp.where((place >= 0) & (place < segments), place, -2)
        columns = columns_ref[span, :]
        tail = columns[:, depth:].astype(jnp.float32)
        vectors = tail[:, :vecs] * jnp.exp2(tail[:, vecs : 2 * vecs])
        ones = jnp.ones((size, 1), jnp.float32)
        blank = jnp.zeros((size, 127 - vecs), jnp.float32)
        right = jnp.concatenate([vectors, ones, blank], axis=1).astype(jnp.bfloat16)
        cosine = lax.dot_general(
            rows_ref[...], columns, (((1,), (1,)), ((), ())), preferred_element_type=jnp.float32
        )
        affinity = jnp.where(row_place == place, 0.0, jnp.exp2(cosine * sharpness))
        total += jnp.dot(
            affinity.astype(jnp.bfloat16), right, preferred_element_type=jnp.float32
        )
    half = vecs // 2
    sums = total.T
    for peer in range(out_ref.shape[0]):
        part = sums[: vecs + 1, peer * width : (peer + 1) * width]
        out_ref[peer, :half, :width] = part[:half]
        out_ref[peer, :half, width:] = part[half:vecs]
        out_ref[peer, half : half + 1, :width] = part[vecs:]
        out_ref[peer, half : half + 1, width:] = part[vecs:]


def finish_kernel(parts_ref, out_ref):
    half, width = out_ref.shape[0] // 2, out_ref.shape[1]
    total = jnp.sum(parts_ref[...], axis=0)
    product = total[:half] / total[half : half + 1]
    out_ref[:half] = product[:, :width]
    out_ref[half:] = product[:, width:]


def shards(embeddings, scale_weights, vectors):
    scales, dim, segments = embeddings.shape
    vecs = vectors.shape[0]
    peers = lax.axis_size(PLANE)
    packed = vecs // 2 + 8
    sharpness = SHARP * math.sqrt(dim) * math.log2(math.e)
    row_copies, item = pl.pallas_call(
        prepare_kernel,
        out_shape=(
            jax.ShapeDtypeStruct((peers, segments, LANES), jnp.bfloat16),
            jax.ShapeDtypeStruct((segments, LANES), jnp.bfloat16),
        ),
        in_specs=[HBM, HBM, HBM],
        out_specs=(HBM, HBM),
        scratch_shapes=[
            pltpu.SMEM((1, scales), jnp.float32),
            pltpu.VMEM((scales, segments, dim), jnp.bfloat16),
            pltpu.VMEM((vecs, segments), jnp.bfloat16),
            pltpu.VMEM((segments, LANES), jnp.bfloat16),
            pltpu.VMEM((segments, LANES), jnp.bfloat16),
            pltpu.SemaphoreType.DMA((2 + segments // PART,)),
            pltpu.SemaphoreType.DMA((segments // PART, peers)),
            pltpu.SemaphoreType.DMA(()),
        ],
        compiler_params=grant(60),
        name="prepare",
    )(scale_weights[None], jnp.swapaxes(embeddings, 1, 2), vectors)
    rows = lax.all_to_all(row_copies, PLANE, 0, 0, tiled=True)
    item = item.astype(jnp.float16).reshape(segments // 8, 8, LANES)
    columns = lax.all_gather(item, LINE, axis=0, tiled=True)
    columns = columns.astype(jnp.bfloat16).reshape(-1, LANES)
    starts = jnp.stack(
        [
            lax.axis_index(PLANE) * segments,
            lax.axis_index(LINE) * segments,
            jnp.int32(segments),
        ]
    )
    row_count, column_count = peers * segments, columns.shape[0]
    sums = pl.pallas_call(
        lambda *refs: tile_kernel(scales * dim, vecs, sharpness, *refs),
        out_shape=jax.ShapeDtypeStruct((peers, packed, 2 * segments), jnp.float32),
        in_specs=[SMEM, VMEM, HBM],
        out_specs=VMEM,
        scratch_shapes=[
            pltpu.VMEM((column_count, LANES), jnp.bfloat16),
            pltpu.SemaphoreType.DMA((column_count // TILE + 1,)),
        ],
        compiler_params=grant(48),
        name="tile",
    )(starts, rows.reshape(row_count, LANES), columns)
    parts = lax.all_to_all(sums, PLANE, 0, 0, tiled=True)
    return pl.pallas_call(
        finish_kernel,
        out_shape=jax.ShapeDtypeStruct((vecs, segments), jnp.float32),
        in_specs=[VMEM],
        out_specs=VMEM,
        compiler_params=grant(2),
        name="finish",
    )(parts)


def solution(mesh):
    torus = Mesh(mesh.devices.reshape(4, 8, 2, 4, 2), AXES)
    return jax.shard_map(
        shards,
        mesh=torus,
        in_specs=(P(None, None, AXES), P(), P(None, AXES)),
        out_specs=P(None, AXES),
        check_vma=False,
    )
```

```python
import math

import jax
import jax.numpy as jnp
from jax import lax
from jax.experimental import pallas as pl
from jax.experimental.pallas import tpu as pltpu
from jax.sharding import Mesh
from jax.sharding import PartitionSpec as P


SHARP = 3.5
AXES = ("y", "zl", "zh", "x", "core")
PLANE = ("y", "x")
LINE = ("zh", "zl")
LANES = 1024
TILE = 512
PART = 32
VMEM = pl.BlockSpec(memory_space=pltpu.VMEM)
HBM = pl.BlockSpec(memory_space=pltpu.HBM)
SMEM = pl.BlockSpec(memory_space=pltpu.SMEM)


def grant(mib):
    return pltpu.CompilerParams(vmem_limit_bytes=mib << 20)


def prepare_kernel(
    weights_hbm, embeddings_hbm, vectors_hbm, rows_hbm, item_hbm,
    weights_ref, embeddings_ref, vectors_ref, row_ref, item_ref, in_sems, out_sems, item_sem
):
    scales, segments, dim = embeddings_ref.shape
    vecs, peers = vectors_ref.shape[0], rows_hbm.shape[0]
    count = segments // PART
    loads = [
        pltpu.make_async_copy(weights_hbm, weights_ref, in_sems.at[0]),
        pltpu.make_async_copy(vectors_hbm, vectors_ref, in_sems.at[1]),
    ] + [
        pltpu.make_async_copy(
            embeddings_hbm.at[:, part * PART : (part + 1) * PART],
            embeddings_ref.at[:, part * PART : (part + 1) * PART],
            in_sems.at[2 + part],
        )
        for part in range(count)
    ]
    for load in loads[2:] + loads[:2]:
        load.start()
    rest = LANES - scales * dim
    row_ref[:, scales * dim :] = jnp.zeros((segments, rest), jnp.bfloat16)
    loads[0].wait()
    stores = []
    for part in range(count):
        loads[2 + part].wait()
        span = slice(part * PART, (part + 1) * PART)
        units, weighted = [], []
        for scale in range(scales):
            values = embeddings_ref[scale, span, :].astype(jnp.float32)
            norm = jnp.sum(values * values, axis=1, keepdims=True) + 1e-06
            unit = (values * lax.rsqrt(norm)).astype(jnp.bfloat16).astype(jnp.float32)
            units.append(unit)
            weighted.append(weights_ref[0, scale] * unit)
        row_ref[span, : scales * dim] = jnp.concatenate(weighted, axis=1).astype(jnp.bfloat16)
        for peer in range(peers):
            store = pltpu.make_async_copy(
                row_ref.at[span], rows_hbm.at[peer, span], out_sems.at[part, peer]
            )
            store.start()
            stores.append(store)
        item_ref[span, : scales * dim] = jnp.concatenate(units, axis=1).astype(jnp.bfloat16)
    loads[1].wait()
    vectors = vectors_ref[...].astype(jnp.float32)
    top = jnp.max(jnp.abs(vectors), axis=1, keepdims=True)
    power = jnp.ceil(jnp.log2(jnp.maximum(top, 2.0**-120)))
    scaled = vectors * jnp.exp2(-power)
    powers = jnp.broadcast_to(power, (vecs, segments))
    extra = jnp.concatenate([scaled, powers], axis=0).T
    if rest > 2 * vecs:
        tail = jnp.zeros((segments, rest - 2 * vecs), jnp.float32)
        extra = jnp.concatenate([extra, tail], axis=1)
    item_ref[:, scales * dim :] = extra.astype(jnp.bfloat16)
    keep = pltpu.make_async_copy(item_ref, item_hbm, item_sem)
    keep.start()
    for store in stores:
        store.wait()
    keep.wait()


def affinity_sums(rows_ref, columns_ref, depth, vecs, sharpness, places):
    total = jnp.zeros((rows_ref.shape[0], 128), jnp.float32)
    for start in range(0, columns_ref.shape[0], TILE):
        columns = columns_ref[start : start + TILE, :]
        tail = columns[:, depth:].astype(jnp.float32)
        vectors = tail[:, :vecs] * jnp.exp2(tail[:, vecs : 2 * vecs])
        ones = jnp.ones((TILE, 1), jnp.float32)
        blank = jnp.zeros((TILE, 127 - vecs), jnp.float32)
        right = jnp.concatenate([vectors, ones, blank], axis=1).astype(jnp.bfloat16)
        cosine = lax.dot_general(
            rows_ref[...], columns, (((1,), (1,)), ((), ())), preferred_element_type=jnp.float32
        )
        affinity = jnp.exp2(cosine * sharpness)
        if places is not None:
            row_place, column_place = places
            affinity = jnp.where(row_place == column_place(start), 0.0, affinity)
        total += jnp.dot(
            affinity.astype(jnp.bfloat16), right, preferred_element_type=jnp.float32
        )
    return total


def own_kernel(depth, vecs, sharpness, starts_ref, rows_ref, columns_ref, out_ref):
    row_start, column_start, segments = starts_ref[0], starts_ref[1], starts_ref[2]
    row_place = lax.broadcasted_iota(jnp.int32, (rows_ref.shape[0], 1), 0) - row_start
    row_place = jnp.where((row_place >= 0) & (row_place < segments), row_place, -1)

    def column_place(start):
        place = lax.broadcasted_iota(jnp.int32, (1, TILE), 1) + (start - column_start)
        return jnp.where((place >= 0) & (place < segments), place, -2)

    out_ref[...] = affinity_sums(
        rows_ref, columns_ref, depth, vecs, sharpness, (row_place, column_place)
    )


def other_kernel(depth, vecs, sharpness, rows_ref, columns_ref, first_ref, out_ref):
    total = affinity_sums(rows_ref, columns_ref, depth, vecs, sharpness, None)
    sums = (first_ref[...] + total).T
    half, width = vecs // 2, out_ref.shape[2] // 2
    for peer in range(out_ref.shape[0]):
        part = sums[: vecs + 1, peer * width : (peer + 1) * width]
        out_ref[peer, :half, :width] = part[:half]
        out_ref[peer, :half, width:] = part[half:vecs]
        out_ref[peer, half : half + 1, :width] = part[vecs:]
        out_ref[peer, half : half + 1, width:] = part[vecs:]


def finish_kernel(parts_ref, out_ref):
    half, width = out_ref.shape[0] // 2, out_ref.shape[1]
    total = jnp.sum(parts_ref[...], axis=0)
    product = total[:half] / total[half : half + 1]
    out_ref[:half] = product[:, :width]
    out_ref[half:] = product[:, width:]


def shards(embeddings, scale_weights, vectors):
    scales, dim, segments = embeddings.shape
    vecs = vectors.shape[0]
    peers = lax.axis_size(PLANE)
    packed = vecs // 2 + 8
    sharpness = SHARP * math.sqrt(dim) * math.log2(math.e)
    row_copies, item = pl.pallas_call(
        prepare_kernel,
        out_shape=(
            jax.ShapeDtypeStruct((peers, segments, LANES), jnp.bfloat16),
            jax.ShapeDtypeStruct((segments, LANES), jnp.bfloat16),
        ),
        in_specs=[HBM, HBM, HBM],
        out_specs=(HBM, HBM),
        scratch_shapes=[
            pltpu.SMEM((1, scales), jnp.float32),
            pltpu.VMEM((scales, segments, dim), jnp.bfloat16),
            pltpu.VMEM((vecs, segments), jnp.bfloat16),
            pltpu.VMEM((segments, LANES), jnp.bfloat16),
            pltpu.VMEM((segments, LANES), jnp.bfloat16),
            pltpu.SemaphoreType.DMA((2 + segments // PART,)),
            pltpu.SemaphoreType.DMA((segments // PART, peers)),
            pltpu.SemaphoreType.DMA(()),
        ],
        compiler_params=grant(60),
        name="prepare",
    )(scale_weights[None], jnp.swapaxes(embeddings, 1, 2), vectors)
    rows = lax.all_to_all(row_copies, PLANE, 0, 0, tiled=True)
    item = item.astype(jnp.float16).reshape(segments // 8, 8, LANES)
    columns = lax.all_gather(item, LINE, axis=0, tiled=True)
    columns = columns.astype(jnp.bfloat16).reshape(-1, LANES)
    others = lax.ppermute(columns, "core", [(0, 1), (1, 0)])
    starts = jnp.stack(
        [
            lax.axis_index(PLANE) * segments,
            lax.axis_index(LINE) * segments,
            jnp.int32(segments),
        ]
    )
    row_count = peers * segments
    rows = rows.reshape(row_count, LANES)
    settings = (scales * dim, vecs, sharpness)
    first = pl.pallas_call(
        lambda *refs: own_kernel(*settings, *refs),
        out_shape=jax.ShapeDtypeStruct((row_count, 128), jnp.float32),
        in_specs=[SMEM, VMEM, VMEM],
        out_specs=VMEM,
        compiler_params=grant(24),
        name="own",
    )(starts, rows, columns)
    sums = pl.pallas_call(
        lambda *refs: other_kernel(*settings, *refs),
        out_shape=jax.ShapeDtypeStruct((peers, packed, 2 * segments), jnp.float32),
        in_specs=[VMEM, VMEM, VMEM],
        out_specs=VMEM,
        compiler_params=grant(24),
        name="other",
    )(rows, others, first)
    parts = lax.all_to_all(sums, PLANE, 0, 0, tiled=True)
    return pl.pallas_call(
        finish_kernel,
        out_shape=jax.ShapeDtypeStruct((vecs, segments), jnp.float32),
        in_specs=[VMEM],
        out_specs=VMEM,
        compiler_params=grant(2),
        name="finish",
    )(parts)


def solution(mesh):
    torus = Mesh(mesh.devices.reshape(4, 8, 2, 4, 2), AXES)
    return jax.shard_map(
        shards,
        mesh=torus,
        in_specs=(P(None, None, AXES), P(), P(None, AXES)),
        out_specs=P(None, AXES),
        check_vma=False,
    )
```

```python
import math

import jax
import jax.numpy as jnp
from jax import lax
from jax.experimental import pallas as pl
from jax.experimental.pallas import tpu as pltpu
from jax.sharding import Mesh
from jax.sharding import PartitionSpec as P

SHARP = 3.5
AXES = ("y", "zl", "zh", "x", "core")
PLANE = ("y", "x")
LINE = ("zh", "zl", "core")
LANES = 1024
TILE = 512
PART = 32
VMEM = pl.BlockSpec(memory_space=pltpu.VMEM)
HBM = pl.BlockSpec(memory_space=pltpu.HBM)
SMEM = pl.BlockSpec(memory_space=pltpu.SMEM)


def grant(mib):
    return pltpu.CompilerParams(vmem_limit_bytes=mib << 20)


def prepare_kernel(
    weights_hbm, embeddings_hbm, vectors_hbm, rows_hbm, item_hbm,
    weights_ref, embeddings_ref, vectors_ref, row_ref, item_ref, in_sems, out_sems, item_sem
):
    scales, segments, dim = embeddings_ref.shape
    vecs, peers = vectors_ref.shape[0], rows_hbm.shape[0]
    count = segments // PART
    loads = [
        pltpu.make_async_copy(weights_hbm, weights_ref, in_sems.at[0]),
        pltpu.make_async_copy(vectors_hbm, vectors_ref, in_sems.at[1]),
    ] + [
        pltpu.make_async_copy(
            embeddings_hbm.at[:, part * PART : (part + 1) * PART],
            embeddings_ref.at[:, part * PART : (part + 1) * PART],
            in_sems.at[2 + part],
        )
        for part in range(count)
    ]
    for load in loads[2:] + loads[:2]:
        load.start()
    rest = LANES - scales * dim
    row_ref[:, scales * dim :] = jnp.zeros((segments, rest), jnp.bfloat16)
    loads[0].wait()
    stores = []
    for part in range(count):
        loads[2 + part].wait()
        span = slice(part * PART, (part + 1) * PART)
        units, weighted = [], []
        for scale in range(scales):
            values = embeddings_ref[scale, span, :].astype(jnp.float32)
            norm = jnp.sum(values * values, axis=1, keepdims=True) + 1e-06
            unit = (values * lax.rsqrt(norm)).astype(jnp.bfloat16).astype(jnp.float32)
            units.append(unit)
            weighted.append(weights_ref[0, scale] * unit)
        row_ref[span, : scales * dim] = jnp.concatenate(weighted, axis=1).astype(jnp.bfloat16)
        for peer in range(peers):
            store = pltpu.make_async_copy(
                row_ref.at[span], rows_hbm.at[peer, span], out_sems.at[part, peer]
            )
            store.start()
            stores.append(store)
        item_ref[span, : scales * dim] = jnp.concatenate(units, axis=1).astype(jnp.bfloat16)
    loads[1].wait()
    vectors = vectors_ref[...].astype(jnp.float32)
    top = jnp.max(jnp.abs(vectors), axis=1, keepdims=True)
    power = jnp.ceil(jnp.log2(jnp.maximum(top, 2.0**-120)))
    scaled = vectors * jnp.exp2(-power)
    powers = jnp.broadcast_to(power, (vecs, segments))
    extra = jnp.concatenate([scaled, powers], axis=0).T
    if rest > 2 * vecs:
        tail = jnp.zeros((segments, rest - 2 * vecs), jnp.float32)
        extra = jnp.concatenate([extra, tail], axis=1)
    item_ref[:, scales * dim :] = extra.astype(jnp.bfloat16)
    keep = pltpu.make_async_copy(item_ref, item_hbm, item_sem)
    keep.start()
    for store in stores:
        store.wait()
    keep.wait()


def tile_kernel(depth, vecs, sharpness, starts_ref, rows_ref, columns_ref, out_ref):
    row_count, column_count = rows_ref.shape[0], columns_ref.shape[0]
    row_start, column_start, segments = starts_ref[0], starts_ref[1], starts_ref[2]
    width = out_ref.shape[2] // 2
    row_place = lax.broadcasted_iota(jnp.int32, (row_count, 1), 0) - row_start
    row_place = jnp.where((row_place >= 0) & (row_place < segments), row_place, -1)
    total = jnp.zeros((row_count, 128), jnp.float32)
    for start in range(0, column_count, TILE):
        place = lax.broadcasted_iota(jnp.int32, (1, TILE), 1) + (start - column_start)
        place = jnp.where((place >= 0) & (place < segments), place, -2)
        columns = columns_ref[start : start + TILE, :]
        tail = columns[:, depth:].astype(jnp.float32)
        vectors = tail[:, :vecs] * jnp.exp2(tail[:, vecs : 2 * vecs])
        ones = jnp.ones((TILE, 1), jnp.float32)
        blank = jnp.zeros((TILE, 127 - vecs), jnp.float32)
        right = jnp.concatenate([vectors, ones, blank], axis=1).astype(jnp.bfloat16)
        cosine = lax.dot_general(
            rows_ref[...], columns, (((1,), (1,)), ((), ())), preferred_element_type=jnp.float32
        )
        affinity = jnp.where(row_place == place, 0.0, jnp.exp2(cosine * sharpness))
        total += jnp.dot(
            affinity.astype(jnp.bfloat16), right, preferred_element_type=jnp.float32
        )
    half = vecs // 2
    sums = total.T
    for peer in range(out_ref.shape[0]):
        part = sums[: vecs + 1, peer * width : (peer + 1) * width]
        out_ref[peer, :half, :width] = part[:half]
        out_ref[peer, :half, width:] = part[half:vecs]
        out_ref[peer, half : half + 1, :width] = part[vecs:]
        out_ref[peer, half : half + 1, width:] = part[vecs:]


def finish_kernel(parts_ref, out_ref):
    half, width = out_ref.shape[0] // 2, out_ref.shape[1]
    total = jnp.sum(parts_ref[...], axis=0)
    product = total[:half] / total[half : half + 1]
    out_ref[:half] = product[:, :width]
    out_ref[half:] = product[:, width:]


def shards(embeddings, scale_weights, vectors):
    scales, dim, segments = embeddings.shape
    vecs = vectors.shape[0]
    peers = lax.axis_size(PLANE)
    packed = vecs // 2 + 8
    sharpness = SHARP * math.sqrt(dim) * math.log2(math.e)
    row_copies, item = pl.pallas_call(
        prepare_kernel,
        out_shape=(
            jax.ShapeDtypeStruct((peers, segments, LANES), jnp.bfloat16),
            jax.ShapeDtypeStruct((segments, LANES), jnp.bfloat16),
        ),
        in_specs=[HBM, HBM, HBM],
        out_specs=(HBM, HBM),
        scratch_shapes=[
            pltpu.SMEM((1, scales), jnp.float32),
            pltpu.VMEM((scales, segments, dim), jnp.bfloat16),
            pltpu.VMEM((vecs, segments), jnp.bfloat16),
            pltpu.VMEM((segments, LANES), jnp.bfloat16),
            pltpu.VMEM((segments, LANES), jnp.bfloat16),
            pltpu.SemaphoreType.DMA((2 + segments // PART,)),
            pltpu.SemaphoreType.DMA((segments // PART, peers)),
            pltpu.SemaphoreType.DMA(()),
        ],
        compiler_params=grant(60),
        name="prepare",
    )(scale_weights[None], jnp.swapaxes(embeddings, 1, 2), vectors)
    rows = lax.all_to_all(row_copies, PLANE, 0, 0, tiled=True)
    item = item.astype(jnp.float16).reshape(segments // 8, 8, LANES)
    columns = lax.all_gather(item, LINE, axis=0, tiled=True)
    rows, columns = lax.optimization_barrier((rows, columns))
    columns = columns.astype(jnp.bfloat16).reshape(-1, LANES)
    starts = jnp.stack(
        [
            lax.axis_index(PLANE) * segments,
            lax.axis_index(LINE) * segments,
            jnp.int32(segments),
        ]
    )
    row_count, column_count = peers * segments, columns.shape[0]
    sums = pl.pallas_call(
        lambda *refs: tile_kernel(scales * dim, vecs, sharpness, *refs),
        out_shape=jax.ShapeDtypeStruct((peers, packed, 2 * segments), jnp.float32),
        in_specs=[SMEM, VMEM, VMEM],
        out_specs=VMEM,
        compiler_params=grant(24),
        name="tile",
    )(starts, rows.reshape(row_count, LANES), columns)
    parts = lax.all_to_all(sums, PLANE, 0, 0, tiled=True)
    return pl.pallas_call(
        finish_kernel,
        out_shape=jax.ShapeDtypeStruct((vecs, segments), jnp.float32),
        in_specs=[VMEM],
        out_specs=VMEM,
        compiler_params=grant(2),
        name="finish",
    )(parts)


def solution(mesh):
    torus = Mesh(mesh.devices.reshape(4, 8, 2, 4, 2), AXES)
    return jax.shard_map(
        shards,
        mesh=torus,
        in_specs=(P(None, None, AXES), P(), P(None, AXES)),
        out_specs=P(None, AXES),
        check_vma=False,
    )
```

```python
import math

import jax
import jax.numpy as jnp
from jax import lax
from jax.experimental import pallas as pl
from jax.experimental.pallas import tpu as pltpu
from jax.sharding import Mesh
from jax.sharding import PartitionSpec as P

SHARP = 3.5
AXES = ("y", "zl", "zh", "x", "core")
PLANE = ("y", "x")
LINE = ("zh", "zl", "core")
LANES = 1024
PART = 32
VMEM = pl.BlockSpec(memory_space=pltpu.VMEM)
HBM = pl.BlockSpec(memory_space=pltpu.HBM)


def grant(mib):
    return pltpu.CompilerParams(vmem_limit_bytes=mib << 20)


def prepare_kernel(
    weights_hbm, embeddings_hbm, vectors_hbm, rows_hbm, item_hbm,
    weights_ref, embeddings_ref, vectors_ref, row_ref, item_ref, in_sems, out_sems, item_sem
):
    scales, segments, dim = embeddings_ref.shape
    vecs, peers = vectors_ref.shape[0], rows_hbm.shape[0]
    count = segments // PART
    loads = [
        pltpu.make_async_copy(weights_hbm, weights_ref, in_sems.at[0]),
        pltpu.make_async_copy(vectors_hbm, vectors_ref, in_sems.at[1]),
    ] + [
        pltpu.make_async_copy(
            embeddings_hbm.at[:, part * PART : (part + 1) * PART],
            embeddings_ref.at[:, part * PART : (part + 1) * PART],
            in_sems.at[2 + part],
        )
        for part in range(count)
    ]
    for load in loads[2:] + loads[:2]:
        load.start()
    rest = LANES - scales * dim
    row_ref[:, scales * dim :] = jnp.zeros((segments, rest), jnp.bfloat16)
    loads[0].wait()
    stores = []
    for part in range(count):
        loads[2 + part].wait()
        span = slice(part * PART, (part + 1) * PART)
        units, weighted = [], []
        for scale in range(scales):
            values = embeddings_ref[scale, span, :].astype(jnp.float32)
            norm = jnp.sum(values * values, axis=1, keepdims=True) + 1e-06
            unit = (values * lax.rsqrt(norm)).astype(jnp.bfloat16).astype(jnp.float32)
            units.append(unit)
            weighted.append(weights_ref[0, scale] * unit)
        row_ref[span, : scales * dim] = jnp.concatenate(weighted, axis=1).astype(jnp.bfloat16)
        for peer in range(peers):
            store = pltpu.make_async_copy(
                row_ref.at[span], rows_hbm.at[peer, span], out_sems.at[part, peer]
            )
            store.start()
            stores.append(store)
        item_ref[span, : scales * dim] = jnp.concatenate(units, axis=1).astype(jnp.bfloat16)
    loads[1].wait()
    vectors = vectors_ref[...].astype(jnp.float32)
    top = jnp.max(jnp.abs(vectors), axis=1, keepdims=True)
    power = jnp.ceil(jnp.log2(jnp.maximum(top, 2.0**-120)))
    scaled = vectors * jnp.exp2(-power)
    powers = jnp.broadcast_to(power, (vecs, segments))
    extra = jnp.concatenate([scaled, powers], axis=0).T
    if rest > 2 * vecs:
        tail = jnp.zeros((segments, rest - 2 * vecs), jnp.float32)
        extra = jnp.concatenate([extra, tail], axis=1)
    item_ref[:, scales * dim :] = extra.astype(jnp.bfloat16)
    keep = pltpu.make_async_copy(item_ref, item_hbm, item_sem)
    keep.start()
    for store in stores:
        store.wait()
    keep.wait()


def sums_kernel(vecs, affinity_ref, tail_ref, out_ref):
    count = tail_ref.shape[0]
    tail = tail_ref[...].astype(jnp.float32)
    vectors = tail[:, :vecs] * jnp.exp2(tail[:, vecs : 2 * vecs])
    ones = jnp.ones((count, 1), jnp.float32)
    blank = jnp.zeros((count, 127 - vecs), jnp.float32)
    right = jnp.concatenate([vectors, ones, blank], axis=1).astype(jnp.bfloat16)
    total = jnp.dot(affinity_ref[...], right, preferred_element_type=jnp.float32)
    sums = total.T
    half, width = vecs // 2, out_ref.shape[2] // 2
    for peer in range(out_ref.shape[0]):
        part = sums[: vecs + 1, peer * width : (peer + 1) * width]
        out_ref[peer, :half, :width] = part[:half]
        out_ref[peer, :half, width:] = part[half:vecs]
        out_ref[peer, half : half + 1, :width] = part[vecs:]
        out_ref[peer, half : half + 1, width:] = part[vecs:]


def places(count, start, segments, outside):
    place = jnp.arange(count, dtype=jnp.int32) - start
    return jnp.where((place >= 0) & (place < segments), place, outside)


def finish_kernel(parts_ref, out_ref):
    half, width = out_ref.shape[0] // 2, out_ref.shape[1]
    total = jnp.sum(parts_ref[...], axis=0)
    product = total[:half] / total[half : half + 1]
    out_ref[:half] = product[:, :width]
    out_ref[half:] = product[:, width:]


def shards(embeddings, scale_weights, vectors):
    scales, dim, segments = embeddings.shape
    vecs = vectors.shape[0]
    peers = lax.axis_size(PLANE)
    packed = vecs // 2 + 8
    sharpness = SHARP * math.sqrt(dim) * math.log2(math.e)
    row_copies, item = pl.pallas_call(
        prepare_kernel,
        out_shape=(
            jax.ShapeDtypeStruct((peers, segments, LANES), jnp.bfloat16),
            jax.ShapeDtypeStruct((segments, LANES), jnp.bfloat16),
        ),
        in_specs=[HBM, HBM, HBM],
        out_specs=(HBM, HBM),
        scratch_shapes=[
            pltpu.SMEM((1, scales), jnp.float32),
            pltpu.VMEM((scales, segments, dim), jnp.bfloat16),
            pltpu.VMEM((vecs, segments), jnp.bfloat16),
            pltpu.VMEM((segments, LANES), jnp.bfloat16),
            pltpu.VMEM((segments, LANES), jnp.bfloat16),
            pltpu.SemaphoreType.DMA((2 + segments // PART,)),
            pltpu.SemaphoreType.DMA((segments // PART, peers)),
            pltpu.SemaphoreType.DMA(()),
        ],
        compiler_params=grant(60),
        name="prepare",
    )(scale_weights[None], jnp.swapaxes(embeddings, 1, 2), vectors)
    rows = lax.all_to_all(row_copies, PLANE, 0, 0, tiled=True)
    item = item.astype(jnp.float16).reshape(segments // 8, 8, LANES)
    columns = lax.all_gather(item, LINE, axis=0, tiled=True)
    rows, columns = lax.optimization_barrier((rows, columns))
    columns = columns.reshape(-1, LANES)
    row_count, column_count = peers * segments, columns.shape[0]
    cosine = lax.dot_general(
        rows.reshape(row_count, LANES),
        columns.astype(jnp.bfloat16),
        (((1,), (1,)), ((), ())),
        preferred_element_type=jnp.float32,
    )
    row_places = places(row_count, lax.axis_index(PLANE) * segments, segments, -1)
    column_places = places(column_count, lax.axis_index(LINE) * segments, segments, -2)
    same = row_places[:, None] == column_places[None, :]
    affinity = jnp.where(same, 0.0, jnp.exp2(cosine * sharpness)).astype(jnp.bfloat16)
    sums = pl.pallas_call(
        lambda *refs: sums_kernel(vecs, *refs),
        out_shape=jax.ShapeDtypeStruct((peers, packed, 2 * segments), jnp.float32),
        in_specs=[VMEM, VMEM],
        out_specs=VMEM,
        compiler_params=grant(16),
        name="sums",
    )(affinity, columns[:, scales * dim :].astype(jnp.bfloat16))
    parts = lax.all_to_all(sums, PLANE, 0, 0, tiled=True)
    return pl.pallas_call(
        finish_kernel,
        out_shape=jax.ShapeDtypeStruct((vecs, segments), jnp.float32),
        in_specs=[VMEM],
        out_specs=VMEM,
        compiler_params=grant(2),
        name="finish",
    )(parts)


def solution(mesh):
    torus = Mesh(mesh.devices.reshape(4, 8, 2, 4, 2), AXES)
    return jax.shard_map(
        shards,
        mesh=torus,
        in_specs=(P(None, None, AXES), P(), P(None, AXES)),
        out_specs=P(None, AXES),
        check_vma=False,
    )
```

```python
import math

import jax
import jax.numpy as jnp
from jax import lax
from jax.experimental import pallas as pl
from jax.experimental.pallas import tpu as pltpu
from jax.sharding import Mesh
from jax.sharding import PartitionSpec as P

SHARP = 3.5
AXES = ("y", "zl", "zh", "x", "core")
PLANE = ("y", "x")
LINE = ("zh", "zl", "core")
LANES = 1024
PART = 32
SMEM = pl.BlockSpec(memory_space=pltpu.SMEM)
VMEM = pl.BlockSpec(memory_space=pltpu.VMEM)
HBM = pl.BlockSpec(memory_space=pltpu.HBM)


def grant(mib):
    return pltpu.CompilerParams(vmem_limit_bytes=mib << 20)


def prepare_kernel(
    weights_hbm, embeddings_hbm, vectors_hbm, rows_hbm, item_hbm,
    weights_ref, embeddings_ref, vectors_ref, row_ref, item_ref, in_sems, out_sems, item_sem
):
    scales, segments, dim = embeddings_ref.shape
    vecs, peers = vectors_ref.shape[0], rows_hbm.shape[0]
    count = segments // PART
    loads = [
        pltpu.make_async_copy(weights_hbm, weights_ref, in_sems.at[0]),
        pltpu.make_async_copy(vectors_hbm, vectors_ref, in_sems.at[1]),
    ] + [
        pltpu.make_async_copy(
            embeddings_hbm.at[:, part * PART : (part + 1) * PART],
            embeddings_ref.at[:, part * PART : (part + 1) * PART],
            in_sems.at[2 + part],
        )
        for part in range(count)
    ]
    for load in loads[2:] + loads[:2]:
        load.start()
    rest = LANES - scales * dim
    row_ref[:, scales * dim :] = jnp.zeros((segments, rest), jnp.bfloat16)
    loads[0].wait()
    stores = []
    for part in range(count):
        loads[2 + part].wait()
        span = slice(part * PART, (part + 1) * PART)
        units, weighted = [], []
        for scale in range(scales):
            values = embeddings_ref[scale, span, :].astype(jnp.float32)
            norm = jnp.sum(values * values, axis=1, keepdims=True) + 1e-06
            unit = (values * lax.rsqrt(norm)).astype(jnp.bfloat16).astype(jnp.float32)
            units.append(unit)
            weighted.append(weights_ref[0, scale] * unit)
        row_ref[span, : scales * dim] = jnp.concatenate(weighted, axis=1).astype(jnp.bfloat16)
        for peer in range(peers):
            store = pltpu.make_async_copy(
                row_ref.at[span], rows_hbm.at[peer, span], out_sems.at[part, peer]
            )
            store.start()
            stores.append(store)
        item_ref[span, : scales * dim] = jnp.concatenate(units, axis=1).astype(jnp.bfloat16)
    loads[1].wait()
    vectors = vectors_ref[...].astype(jnp.float32)
    top = jnp.max(jnp.abs(vectors), axis=1, keepdims=True)
    power = jnp.ceil(jnp.log2(jnp.maximum(top, 2.0**-120)))
    scaled = vectors * jnp.exp2(-power)
    powers = jnp.broadcast_to(power, (vecs, segments))
    extra = jnp.concatenate([scaled, powers], axis=0).T
    if rest > 2 * vecs:
        tail = jnp.zeros((segments, rest - 2 * vecs), jnp.float32)
        extra = jnp.concatenate([extra, tail], axis=1)
    item_ref[:, scales * dim :] = extra.astype(jnp.bfloat16)
    keep = pltpu.make_async_copy(item_ref, item_hbm, item_sem)
    keep.start()
    for store in stores:
        store.wait()
    keep.wait()


def sums_kernel(vecs, width, starts_ref, affinity_ref, tail_ref, out_ref, total_ref):
    count = tail_ref.shape[0]
    tail = tail_ref[...].astype(jnp.float32)
    vectors = tail[:, :vecs] * jnp.exp2(tail[:, vecs : 2 * vecs])
    ones = jnp.ones((count, 1), jnp.float32)
    blank = jnp.zeros((count, 127 - vecs), jnp.float32)
    right = jnp.concatenate([vectors, ones, blank], axis=1).astype(jnp.bfloat16)
    total_ref[...] = jnp.dot(affinity_ref[...], right, preferred_element_type=jnp.float32)
    own = pl.ds(pl.multiple_of(starts_ref[0], width), width)
    row_place = lax.broadcasted_iota(jnp.int32, (width, 1), 0)
    column_place = lax.broadcasted_iota(jnp.int32, (1, count), 1) - starts_ref[1]
    kept = jnp.where(row_place == column_place, 0.0, affinity_ref[own, :].astype(jnp.float32))
    total_ref[own, :] = jnp.dot(
        kept.astype(jnp.bfloat16), right, preferred_element_type=jnp.float32
    )
    sums = total_ref[...].T
    half = vecs // 2
    for peer in range(out_ref.shape[0]):
        part = sums[: vecs + 1, peer * width : (peer + 1) * width]
        out_ref[peer, :half, :width] = part[:half]
        out_ref[peer, :half, width:] = part[half:vecs]
        out_ref[peer, half : half + 1, :width] = part[vecs:]
        out_ref[peer, half : half + 1, width:] = part[vecs:]


def finish_kernel(parts_ref, out_ref):
    half, width = out_ref.shape[0] // 2, out_ref.shape[1]
    total = jnp.sum(parts_ref[...], axis=0)
    product = total[:half] / total[half : half + 1]
    out_ref[:half] = product[:, :width]
    out_ref[half:] = product[:, width:]


def shards(embeddings, scale_weights, vectors):
    scales, dim, segments = embeddings.shape
    vecs = vectors.shape[0]
    peers = lax.axis_size(PLANE)
    packed = vecs // 2 + 8
    sharpness = SHARP * math.sqrt(dim) * math.log2(math.e)
    row_copies, item = pl.pallas_call(
        prepare_kernel,
        out_shape=(
            jax.ShapeDtypeStruct((peers, segments, LANES), jnp.bfloat16),
            jax.ShapeDtypeStruct((segments, LANES), jnp.bfloat16),
        ),
        in_specs=[HBM, HBM, HBM],
        out_specs=(HBM, HBM),
        scratch_shapes=[
            pltpu.SMEM((1, scales), jnp.float32),
            pltpu.VMEM((scales, segments, dim), jnp.bfloat16),
            pltpu.VMEM((vecs, segments), jnp.bfloat16),
            pltpu.VMEM((segments, LANES), jnp.bfloat16),
            pltpu.VMEM((segments, LANES), jnp.bfloat16),
            pltpu.SemaphoreType.DMA((2 + segments // PART,)),
            pltpu.SemaphoreType.DMA((segments // PART, peers)),
            pltpu.SemaphoreType.DMA(()),
        ],
        compiler_params=grant(60),
        name="prepare",
    )(scale_weights[None], jnp.swapaxes(embeddings, 1, 2), vectors)
    rows = lax.all_to_all(row_copies, PLANE, 0, 0, tiled=True)
    item = item.astype(jnp.float16).reshape(segments // 8, 8, LANES)
    columns = lax.all_gather(item, LINE, axis=0, tiled=True)
    columns = columns.reshape(-1, LANES)
    row_count = peers * segments
    cosine = lax.dot_general(
        rows.reshape(row_count, LANES),
        columns.astype(jnp.bfloat16),
        (((1,), (1,)), ((), ())),
        preferred_element_type=jnp.float32,
    )
    affinity = jnp.exp2(cosine * sharpness).astype(jnp.bfloat16)
    starts = jnp.stack([lax.axis_index(PLANE) * segments, lax.axis_index(LINE) * segments])
    sums = pl.pallas_call(
        lambda *refs: sums_kernel(vecs, segments, *refs),
        out_shape=jax.ShapeDtypeStruct((peers, packed, 2 * segments), jnp.float32),
        in_specs=[SMEM, VMEM, VMEM],
        out_specs=VMEM,
        scratch_shapes=[pltpu.VMEM((row_count, 128), jnp.float32)],
        compiler_params=grant(16),
        name="sums",
    )(starts, affinity, columns[:, scales * dim :].astype(jnp.bfloat16))
    parts = lax.all_to_all(sums, PLANE, 0, 0, tiled=True)
    return pl.pallas_call(
        finish_kernel,
        out_shape=jax.ShapeDtypeStruct((vecs, segments), jnp.float32),
        in_specs=[VMEM],
        out_specs=VMEM,
        compiler_params=grant(2),
        name="finish",
    )(parts)


def solution(mesh):
    torus = Mesh(mesh.devices.reshape(4, 8, 2, 4, 2), AXES)
    return jax.shard_map(
        shards,
        mesh=torus,
        in_specs=(P(None, None, AXES), P(), P(None, AXES)),
        out_specs=P(None, AXES),
        check_vma=False,
    )
```

```python
import math

import jax
import jax.numpy as jnp
from jax import lax
from jax.experimental import pallas as pl
from jax.experimental.pallas import tpu as pltpu
from jax.sharding import Mesh
from jax.sharding import PartitionSpec as P

SHARP = 3.5
AXES = ("y", "zl", "zh", "x", "core")
PLANE = ("y", "x")
LINE = ("zh", "zl", "core")
LANES = 1024
PART = 32
NEAR = 768
SMEM = pl.BlockSpec(memory_space=pltpu.SMEM)
VMEM = pl.BlockSpec(memory_space=pltpu.VMEM)
HBM = pl.BlockSpec(memory_space=pltpu.HBM)


def grant(mib):
    return pltpu.CompilerParams(vmem_limit_bytes=mib << 20)


def prepare_kernel(
    weights_hbm, embeddings_hbm, vectors_hbm, rows_hbm, item_hbm,
    weights_ref, embeddings_ref, vectors_ref, row_ref, item_ref, in_sems, out_sems, item_sem
):
    scales, segments, dim = embeddings_ref.shape
    vecs, peers = vectors_ref.shape[0], rows_hbm.shape[0]
    count = segments // PART
    loads = [
        pltpu.make_async_copy(weights_hbm, weights_ref, in_sems.at[0]),
        pltpu.make_async_copy(vectors_hbm, vectors_ref, in_sems.at[1]),
    ] + [
        pltpu.make_async_copy(
            embeddings_hbm.at[:, part * PART : (part + 1) * PART],
            embeddings_ref.at[:, part * PART : (part + 1) * PART],
            in_sems.at[2 + part],
        )
        for part in range(count)
    ]
    for load in loads[2:] + loads[:2]:
        load.start()
    rest = LANES - scales * dim
    row_ref[:, scales * dim :] = jnp.zeros((segments, rest), jnp.bfloat16)
    loads[0].wait()
    stores = []
    for part in range(count):
        loads[2 + part].wait()
        span = slice(part * PART, (part + 1) * PART)
        units, weighted = [], []
        for scale in range(scales):
            values = embeddings_ref[scale, span, :].astype(jnp.float32)
            norm = jnp.sum(values * values, axis=1, keepdims=True) + 1e-06
            unit = (values * lax.rsqrt(norm)).astype(jnp.bfloat16).astype(jnp.float32)
            units.append(unit)
            weighted.append(weights_ref[0, scale] * unit)
        row_ref[span, : scales * dim] = jnp.concatenate(weighted, axis=1).astype(jnp.bfloat16)
        for peer in range(peers):
            store = pltpu.make_async_copy(
                row_ref.at[span], rows_hbm.at[peer, span], out_sems.at[part, peer]
            )
            store.start()
            stores.append(store)
        item_ref[span, : scales * dim] = jnp.concatenate(units, axis=1).astype(jnp.bfloat16)
    loads[1].wait()
    vectors = vectors_ref[...].astype(jnp.float32)
    top = jnp.max(jnp.abs(vectors), axis=1, keepdims=True)
    power = jnp.ceil(jnp.log2(jnp.maximum(top, 2.0**-120)))
    scaled = vectors * jnp.exp2(-power)
    powers = jnp.broadcast_to(power, (vecs, segments))
    extra = jnp.concatenate([scaled, powers], axis=0).T
    if rest > 2 * vecs:
        tail = jnp.zeros((segments, rest - 2 * vecs), jnp.float32)
        extra = jnp.concatenate([extra, tail], axis=1)
    item_ref[:, scales * dim :] = extra.astype(jnp.bfloat16)
    keep = pltpu.make_async_copy(item_ref, item_hbm, item_sem)
    keep.start()
    for store in stores:
        store.wait()
    keep.wait()


def sums_kernel(vecs, width, starts_ref, near_in, far_in, tail_ref, out_ref, near_ref, far_ref):
    tail = tail_ref[...].astype(jnp.float32)
    count, lanes = tail_ref.shape[0], 2 * width
    row_start, column_start = starts_ref[0], starts_ref[1]
    rows = pl.ds(pl.multiple_of(row_start, width), width)

    def clear_diagonal(part_ref, start, size):
        @pl.when((column_start >= start) & (column_start < start + size))
        def _():
            place = column_start - start
            base = pl.multiple_of(place // lanes * lanes, lanes)
            block = part_ref[rows, pl.ds(base, lanes)].astype(jnp.float32)
            row_place = lax.broadcasted_iota(jnp.int32, block.shape, 0)
            column_place = lax.broadcasted_iota(jnp.int32, block.shape, 1) + (base - place)
            kept = jnp.where(row_place == column_place, 0.0, block)
            part_ref[rows, pl.ds(base, lanes)] = kept.astype(jnp.bfloat16)

    near = near_ref.shape[1]
    clear_diagonal(near_ref, 0, near)
    clear_diagonal(far_ref, near, count - near)
    vectors = tail[:, :vecs] * jnp.exp2(tail[:, vecs : 2 * vecs])
    ones = jnp.ones((count, 1), jnp.float32)
    blank = jnp.zeros((count, 127 - vecs), jnp.float32)
    right = jnp.concatenate([vectors, ones, blank], axis=1).astype(jnp.bfloat16)
    total = jnp.dot(near_ref[...], right[:near], preferred_element_type=jnp.float32)
    total += jnp.dot(far_ref[...], right[near:], preferred_element_type=jnp.float32)
    sums = total.T
    half = vecs // 2
    for peer in range(out_ref.shape[0]):
        part = sums[: vecs + 1, peer * width : (peer + 1) * width]
        out_ref[peer, :half, :width] = part[:half]
        out_ref[peer, :half, width:] = part[half:vecs]
        out_ref[peer, half : half + 1, :width] = part[vecs:]
        out_ref[peer, half : half + 1, width:] = part[vecs:]


def finish_kernel(parts_ref, out_ref):
    half, width = out_ref.shape[0] // 2, out_ref.shape[1]
    total = jnp.sum(parts_ref[...], axis=0)
    product = total[:half] / total[half : half + 1]
    out_ref[:half] = product[:, :width]
    out_ref[half:] = product[:, width:]


def shards(embeddings, scale_weights, vectors):
    scales, dim, segments = embeddings.shape
    vecs = vectors.shape[0]
    peers = lax.axis_size(PLANE)
    packed = vecs // 2 + 8
    sharpness = SHARP * math.sqrt(dim) * math.log2(math.e)
    row_copies, item = pl.pallas_call(
        prepare_kernel,
        out_shape=(
            jax.ShapeDtypeStruct((peers, segments, LANES), jnp.bfloat16),
            jax.ShapeDtypeStruct((segments, LANES), jnp.bfloat16),
        ),
        in_specs=[HBM, HBM, HBM],
        out_specs=(HBM, HBM),
        scratch_shapes=[
            pltpu.SMEM((1, scales), jnp.float32),
            pltpu.VMEM((scales, segments, dim), jnp.bfloat16),
            pltpu.VMEM((vecs, segments), jnp.bfloat16),
            pltpu.VMEM((segments, LANES), jnp.bfloat16),
            pltpu.VMEM((segments, LANES), jnp.bfloat16),
            pltpu.SemaphoreType.DMA((2 + segments // PART,)),
            pltpu.SemaphoreType.DMA((segments // PART, peers)),
            pltpu.SemaphoreType.DMA(()),
        ],
        compiler_params=grant(60),
        name="prepare",
    )(scale_weights[None], jnp.swapaxes(embeddings, 1, 2), vectors)
    rows = lax.all_to_all(row_copies, PLANE, 0, 0, tiled=True)
    item = item.astype(jnp.float16).reshape(segments // 8, 8, LANES)
    columns = lax.all_gather(item, LINE, axis=0, tiled=True)
    rows, columns = lax.optimization_barrier((rows, columns))
    columns = columns.reshape(-1, LANES)
    row_count = peers * segments
    rows = rows.reshape(row_count, LANES)

    def affinity_to(part):
        cosine = lax.dot_general(
            rows,
            part.astype(jnp.bfloat16),
            (((1,), (1,)), ((), ())),
            preferred_element_type=jnp.float32,
        )
        return jnp.exp2(cosine * sharpness).astype(jnp.bfloat16)

    near = affinity_to(columns[:NEAR])
    near, late = lax.optimization_barrier((near, columns))
    far = affinity_to(late[NEAR:])
    starts = jnp.stack([lax.axis_index(PLANE) * segments, lax.axis_index(LINE) * segments])
    sums, _, _ = pl.pallas_call(
        lambda *refs: sums_kernel(vecs, segments, *refs),
        out_shape=(
            jax.ShapeDtypeStruct((peers, packed, 2 * segments), jnp.float32),
            jax.ShapeDtypeStruct(near.shape, near.dtype),
            jax.ShapeDtypeStruct(far.shape, far.dtype),
        ),
        in_specs=[SMEM, VMEM, VMEM, VMEM],
        out_specs=(VMEM, VMEM, VMEM),
        input_output_aliases={1: 1, 2: 2},
        compiler_params=grant(16),
        name="sums",
    )(starts, near, far, columns[:, scales * dim :].astype(jnp.bfloat16))
    parts = lax.all_to_all(sums, PLANE, 0, 0, tiled=True)
    return pl.pallas_call(
        finish_kernel,
        out_shape=jax.ShapeDtypeStruct((vecs, segments), jnp.float32),
        in_specs=[VMEM],
        out_specs=VMEM,
        compiler_params=grant(2),
        name="finish",
    )(parts)


def solution(mesh):
    torus = Mesh(mesh.devices.reshape(4, 8, 2, 4, 2), AXES)
    return jax.shard_map(
        shards,
        mesh=torus,
        in_specs=(P(None, None, AXES), P(), P(None, AXES)),
        out_specs=P(None, AXES),
        check_vma=False,
    )
```

```python
import math

import jax
import jax.numpy as jnp
from jax import lax
from jax.experimental import pallas as pl
from jax.experimental.pallas import tpu as pltpu
from jax.sharding import Mesh
from jax.sharding import PartitionSpec as P

SHARP = 3.5
AXES = ("y", "zl", "zh", "x", "core")
PLANE = ("y", "x")
LINE = ("zh", "zl", "core")
LANES = 1024
PART = 32
NEAR = 1024
SMEM = pl.BlockSpec(memory_space=pltpu.SMEM)
VMEM = pl.BlockSpec(memory_space=pltpu.VMEM)
HBM = pl.BlockSpec(memory_space=pltpu.HBM)


def grant(mib):
    return pltpu.CompilerParams(vmem_limit_bytes=mib << 20)


def prepare_kernel(
    weights_hbm, embeddings_hbm, vectors_hbm, rows_hbm, item_hbm,
    weights_ref, embeddings_ref, vectors_ref, row_ref, item_ref, in_sems, out_sems, item_sem
):
    scales, segments, dim = embeddings_ref.shape
    vecs, peers = vectors_ref.shape[0], rows_hbm.shape[0]
    count = segments // PART
    loads = [
        pltpu.make_async_copy(weights_hbm, weights_ref, in_sems.at[0]),
        pltpu.make_async_copy(vectors_hbm, vectors_ref, in_sems.at[1]),
    ] + [
        pltpu.make_async_copy(
            embeddings_hbm.at[:, part * PART : (part + 1) * PART],
            embeddings_ref.at[:, part * PART : (part + 1) * PART],
            in_sems.at[2 + part],
        )
        for part in range(count)
    ]
    for load in loads[2:] + loads[:2]:
        load.start()
    rest = LANES - scales * dim
    row_ref[:, scales * dim :] = jnp.zeros((segments, rest), jnp.bfloat16)
    loads[0].wait()
    stores = []
    for part in range(count):
        loads[2 + part].wait()
        span = slice(part * PART, (part + 1) * PART)
        units, weighted = [], []
        for scale in range(scales):
            values = embeddings_ref[scale, span, :].astype(jnp.float32)
            norm = jnp.sum(values * values, axis=1, keepdims=True) + 1e-06
            unit = (values * lax.rsqrt(norm)).astype(jnp.bfloat16).astype(jnp.float32)
            units.append(unit)
            weighted.append(weights_ref[0, scale] * unit)
        row_ref[span, : scales * dim] = jnp.concatenate(weighted, axis=1).astype(jnp.bfloat16)
        for peer in range(peers):
            store = pltpu.make_async_copy(
                row_ref.at[span], rows_hbm.at[peer, span], out_sems.at[part, peer]
            )
            store.start()
            stores.append(store)
        item_ref[span, : scales * dim] = jnp.concatenate(units, axis=1).astype(jnp.bfloat16)
    loads[1].wait()
    vectors = vectors_ref[...].astype(jnp.float32)
    top = jnp.max(jnp.abs(vectors), axis=1, keepdims=True)
    power = jnp.ceil(jnp.log2(jnp.maximum(top, 2.0**-120)))
    scaled = vectors * jnp.exp2(-power)
    powers = jnp.broadcast_to(power, (vecs, segments))
    extra = jnp.concatenate([scaled, powers], axis=0).T
    if rest > 2 * vecs:
        tail = jnp.zeros((segments, rest - 2 * vecs), jnp.float32)
        extra = jnp.concatenate([extra, tail], axis=1)
    item_ref[:, scales * dim :] = extra.astype(jnp.bfloat16)
    keep = pltpu.make_async_copy(item_ref, item_hbm, item_sem)
    keep.start()
    for store in stores:
        store.wait()
    keep.wait()


def sums_kernel(vecs, width, starts_ref, near_in, far_in, tail_ref, out_ref, near_ref, far_ref):
    tail = tail_ref[...].astype(jnp.float32)
    count, lanes = tail_ref.shape[0], 2 * width
    row_start, column_start = starts_ref[0], starts_ref[1]
    rows = pl.ds(pl.multiple_of(row_start, width), width)

    def clear_diagonal(part_ref, start, size):
        @pl.when((column_start >= start) & (column_start < start + size))
        def _():
            place = column_start - start
            base = pl.multiple_of(place // lanes * lanes, lanes)
            block = part_ref[rows, pl.ds(base, lanes)].astype(jnp.float32)
            row_place = lax.broadcasted_iota(jnp.int32, block.shape, 0)
            column_place = lax.broadcasted_iota(jnp.int32, block.shape, 1) + (base - place)
            kept = jnp.where(row_place == column_place, 0.0, block)
            part_ref[rows, pl.ds(base, lanes)] = kept.astype(jnp.bfloat16)

    near = near_ref.shape[1]
    clear_diagonal(near_ref, 0, near)
    clear_diagonal(far_ref, near, count - near)
    vectors = tail[:, :vecs] * jnp.exp2(tail[:, vecs : 2 * vecs])
    ones = jnp.ones((count, 1), jnp.float32)
    blank = jnp.zeros((count, 127 - vecs), jnp.float32)
    right = jnp.concatenate([vectors, ones, blank], axis=1).astype(jnp.bfloat16)
    total = jnp.dot(near_ref[...], right[:near], preferred_element_type=jnp.float32)
    total += jnp.dot(far_ref[...], right[near:], preferred_element_type=jnp.float32)
    sums = total.T[: vecs + 1].astype(jnp.bfloat16)
    half = vecs // 2
    for peer in range(out_ref.shape[0]):
        part = sums[:, peer * width : (peer + 1) * width]
        out_ref[peer, :half, :width] = part[:half]
        out_ref[peer, :half, width:] = part[half:vecs]
        out_ref[peer, half : half + 1, :width] = part[vecs:]
        out_ref[peer, half : half + 1, width:] = part[vecs:]


def finish_kernel(parts_ref, out_ref):
    half, width = out_ref.shape[0] // 2, out_ref.shape[1]
    total = jnp.sum(parts_ref[...].astype(jnp.float32), axis=0)
    product = total[:half] / total[half : half + 1]
    out_ref[:half] = product[:, :width]
    out_ref[half:] = product[:, width:]


def shards(embeddings, scale_weights, vectors):
    scales, dim, segments = embeddings.shape
    vecs = vectors.shape[0]
    peers = lax.axis_size(PLANE)
    packed = vecs // 2 + 8
    sharpness = SHARP * math.sqrt(dim) * math.log2(math.e)
    row_copies, item = pl.pallas_call(
        prepare_kernel,
        out_shape=(
            jax.ShapeDtypeStruct((peers, segments, LANES), jnp.bfloat16),
            jax.ShapeDtypeStruct((segments, LANES), jnp.bfloat16),
        ),
        in_specs=[HBM, HBM, HBM],
        out_specs=(HBM, HBM),
        scratch_shapes=[
            pltpu.SMEM((1, scales), jnp.float32),
            pltpu.VMEM((scales, segments, dim), jnp.bfloat16),
            pltpu.VMEM((vecs, segments), jnp.bfloat16),
            pltpu.VMEM((segments, LANES), jnp.bfloat16),
            pltpu.VMEM((segments, LANES), jnp.bfloat16),
            pltpu.SemaphoreType.DMA((2 + segments // PART,)),
            pltpu.SemaphoreType.DMA((segments // PART, peers)),
            pltpu.SemaphoreType.DMA(()),
        ],
        compiler_params=grant(60),
        name="prepare",
    )(scale_weights[None], jnp.swapaxes(embeddings, 1, 2), vectors)
    rows = lax.all_to_all(row_copies, PLANE, 0, 0, tiled=True)
    item = item.astype(jnp.float16).reshape(segments // 8, 8, LANES)
    columns = lax.all_gather(item, LINE, axis=0, tiled=True)
    rows, columns = lax.optimization_barrier((rows, columns))
    columns = columns.reshape(-1, LANES)
    row_count = peers * segments
    rows = rows.reshape(row_count, LANES)

    def affinity_to(part):
        cosine = lax.dot_general(
            rows,
            part.astype(jnp.bfloat16),
            (((1,), (1,)), ((), ())),
            preferred_element_type=jnp.float32,
        )
        return jnp.exp2(cosine * sharpness).astype(jnp.bfloat16)

    near = affinity_to(columns[:NEAR])
    near, late = lax.optimization_barrier((near, columns))
    far = affinity_to(late[NEAR:])
    starts = jnp.stack([lax.axis_index(PLANE) * segments, lax.axis_index(LINE) * segments])
    sums, _, _ = pl.pallas_call(
        lambda *refs: sums_kernel(vecs, segments, *refs),
        out_shape=(
            jax.ShapeDtypeStruct((peers, packed, 2 * segments), jnp.bfloat16),
            jax.ShapeDtypeStruct(near.shape, near.dtype),
            jax.ShapeDtypeStruct(far.shape, far.dtype),
        ),
        in_specs=[SMEM, VMEM, VMEM, VMEM],
        out_specs=(VMEM, VMEM, VMEM),
        input_output_aliases={1: 1, 2: 2},
        compiler_params=grant(16),
        name="sums",
    )(starts, near, far, columns[:, scales * dim :].astype(jnp.bfloat16))
    parts = lax.all_to_all(sums, PLANE, 0, 0, tiled=True)
    return pl.pallas_call(
        finish_kernel,
        out_shape=jax.ShapeDtypeStruct((vecs, segments), jnp.float32),
        in_specs=[VMEM],
        out_specs=VMEM,
        compiler_params=grant(2),
        name="finish",
    )(parts)


def solution(mesh):
    torus = Mesh(mesh.devices.reshape(4, 8, 2, 4, 2), AXES)
    return jax.shard_map(
        shards,
        mesh=torus,
        in_specs=(P(None, None, AXES), P(), P(None, AXES)),
        out_specs=P(None, AXES),
        check_vma=False,
    )
```

```python
import math

import jax
import jax.numpy as jnp
from jax import lax
from jax.experimental import pallas as pl
from jax.experimental.pallas import tpu as pltpu
from jax.sharding import Mesh
from jax.sharding import PartitionSpec as P

SHARP = 3.5
AXES = ("y", "zl", "zh", "x", "core")
PLANE = ("y", "x")
LINE = ("zh", "zl", "core")
LANES = 1024
PART = 32
NEAR = 1024
SMEM = pl.BlockSpec(memory_space=pltpu.SMEM)
VMEM = pl.BlockSpec(memory_space=pltpu.VMEM)
HBM = pl.BlockSpec(memory_space=pltpu.HBM)


def grant(mib):
    return pltpu.CompilerParams(vmem_limit_bytes=mib << 20)


def prepare_kernel(
    weights_hbm, embeddings_hbm, vectors_hbm, rows_hbm, item_hbm,
    weights_ref, embeddings_ref, vectors_ref, row_ref, item_ref, in_sems, out_sems, item_sem
):
    scales, segments, dim = embeddings_ref.shape
    vecs, peers = vectors_ref.shape[0], rows_hbm.shape[0]
    count = segments // PART
    loads = [
        pltpu.make_async_copy(weights_hbm, weights_ref, in_sems.at[0]),
        pltpu.make_async_copy(vectors_hbm, vectors_ref, in_sems.at[1]),
    ] + [
        pltpu.make_async_copy(
            embeddings_hbm.at[:, part * PART : (part + 1) * PART],
            embeddings_ref.at[:, part * PART : (part + 1) * PART],
            in_sems.at[2 + part],
        )
        for part in range(count)
    ]
    for load in loads[2:] + loads[:2]:
        load.start()
    rest = LANES - scales * dim
    row_ref[:, scales * dim :] = jnp.zeros((segments, rest), jnp.bfloat16)
    loads[0].wait()
    stores = []
    for part in range(count):
        loads[2 + part].wait()
        span = slice(part * PART, (part + 1) * PART)
        units, weighted = [], []
        for scale in range(scales):
            values = embeddings_ref[scale, span, :].astype(jnp.float32)
            norm = jnp.sum(values * values, axis=1, keepdims=True) + 1e-06
            unit = (values * lax.rsqrt(norm)).astype(jnp.bfloat16).astype(jnp.float32)
            units.append(unit)
            weighted.append(weights_ref[0, scale] * unit)
        row_ref[span, : scales * dim] = jnp.concatenate(weighted, axis=1).astype(jnp.bfloat16)
        for peer in range(peers):
            store = pltpu.make_async_copy(
                row_ref.at[span], rows_hbm.at[peer, span], out_sems.at[part, peer]
            )
            store.start()
            stores.append(store)
        item_ref[span, : scales * dim] = jnp.concatenate(units, axis=1).astype(jnp.bfloat16)
    loads[1].wait()
    vectors = vectors_ref[...].astype(jnp.float32)
    top = jnp.max(jnp.abs(vectors), axis=1, keepdims=True)
    power = jnp.ceil(jnp.log2(jnp.maximum(top, 2.0**-120)))
    scaled = vectors * jnp.exp2(-power)
    powers = jnp.broadcast_to(power, (vecs, segments))
    extra = jnp.concatenate([scaled, powers], axis=0).T
    if rest > 2 * vecs:
        tail = jnp.zeros((segments, rest - 2 * vecs), jnp.float32)
        extra = jnp.concatenate([extra, tail], axis=1)
    item_ref[:, scales * dim :] = extra.astype(jnp.bfloat16)
    keep = pltpu.make_async_copy(item_ref, item_hbm, item_sem)
    keep.start()
    for store in stores:
        store.wait()
    keep.wait()


def right_kernel(vecs, tail_ref, right_ref):
    tail = tail_ref[...].astype(jnp.float32)
    vectors = tail[:, :vecs] * jnp.exp2(tail[:, vecs : 2 * vecs])
    ones = jnp.ones((tail.shape[0], 1), jnp.float32)
    blank = jnp.zeros((tail.shape[0], 127 - vecs), jnp.float32)
    right_ref[...] = jnp.concatenate([vectors, ones, blank], axis=1).astype(jnp.bfloat16)


def sums_kernel(vecs, width, starts_ref, near_in, far_in, right_ref, out_ref, near_ref, far_ref):
    count, lanes = right_ref.shape[0], 2 * width
    row_start, column_start = starts_ref[0], starts_ref[1]
    rows = pl.ds(pl.multiple_of(row_start, width), width)

    def clear_diagonal(part_ref, start, size):
        @pl.when((column_start >= start) & (column_start < start + size))
        def _():
            place = column_start - start
            base = pl.multiple_of(place // lanes * lanes, lanes)
            block = part_ref[rows, pl.ds(base, lanes)].astype(jnp.float32)
            row_place = lax.broadcasted_iota(jnp.int32, block.shape, 0)
            column_place = lax.broadcasted_iota(jnp.int32, block.shape, 1) + (base - place)
            kept = jnp.where(row_place == column_place, 0.0, block)
            part_ref[rows, pl.ds(base, lanes)] = kept.astype(jnp.bfloat16)

    near = near_ref.shape[1]
    clear_diagonal(near_ref, 0, near)
    clear_diagonal(far_ref, near, count - near)
    total = jnp.dot(near_ref[...], right_ref[:near, :], preferred_element_type=jnp.float32)
    total += jnp.dot(far_ref[...], right_ref[near:, :], preferred_element_type=jnp.float32)
    sums = total.T[: vecs + 1].astype(jnp.bfloat16)
    half = vecs // 2
    for peer in range(out_ref.shape[0]):
        part = sums[:, peer * width : (peer + 1) * width]
        out_ref[peer, :half, :width] = part[:half]
        out_ref[peer, :half, width:] = part[half:vecs]
        out_ref[peer, half : half + 1, :width] = part[vecs:]
        out_ref[peer, half : half + 1, width:] = part[vecs:]


def finish_kernel(parts_ref, out_ref):
    half, width = out_ref.shape[0] // 2, out_ref.shape[1]
    total = jnp.sum(parts_ref[...].astype(jnp.float32), axis=0)
    product = total[:half] / total[half : half + 1]
    out_ref[:half] = product[:, :width]
    out_ref[half:] = product[:, width:]


def shards(embeddings, scale_weights, vectors):
    scales, dim, segments = embeddings.shape
    vecs = vectors.shape[0]
    peers = lax.axis_size(PLANE)
    packed = vecs // 2 + 8
    sharpness = SHARP * math.sqrt(dim) * math.log2(math.e)
    row_copies, item = pl.pallas_call(
        prepare_kernel,
        out_shape=(
            jax.ShapeDtypeStruct((peers, segments, LANES), jnp.bfloat16),
            jax.ShapeDtypeStruct((segments, LANES), jnp.bfloat16),
        ),
        in_specs=[HBM, HBM, HBM],
        out_specs=(HBM, HBM),
        scratch_shapes=[
            pltpu.SMEM((1, scales), jnp.float32),
            pltpu.VMEM((scales, segments, dim), jnp.bfloat16),
            pltpu.VMEM((vecs, segments), jnp.bfloat16),
            pltpu.VMEM((segments, LANES), jnp.bfloat16),
            pltpu.VMEM((segments, LANES), jnp.bfloat16),
            pltpu.SemaphoreType.DMA((2 + segments // PART,)),
            pltpu.SemaphoreType.DMA((segments // PART, peers)),
            pltpu.SemaphoreType.DMA(()),
        ],
        compiler_params=grant(60),
        name="prepare",
    )(scale_weights[None], jnp.swapaxes(embeddings, 1, 2), vectors)
    rows = lax.all_to_all(row_copies, PLANE, 0, 0, tiled=True)
    item = item.astype(jnp.float16).reshape(segments // 8, 8, LANES)
    columns = lax.all_gather(item, LINE, axis=0, tiled=True)
    columns = columns.reshape(-1, LANES)
    row_count = peers * segments
    rows = rows.reshape(row_count, LANES)
    right = pl.pallas_call(
        lambda *refs: right_kernel(vecs, *refs),
        out_shape=jax.ShapeDtypeStruct((columns.shape[0], 128), jnp.bfloat16),
        in_specs=[VMEM],
        out_specs=VMEM,
        compiler_params=grant(4),
        name="right",
    )(columns[:, scales * dim :].astype(jnp.bfloat16))

    def affinity_to(part):
        cosine = lax.dot_general(
            rows,
            part.astype(jnp.bfloat16),
            (((1,), (1,)), ((), ())),
            preferred_element_type=jnp.float32,
        )
        return jnp.exp2(cosine * sharpness).astype(jnp.bfloat16)

    near = affinity_to(columns[:NEAR])
    near, late = lax.optimization_barrier((near, columns))
    far = affinity_to(late[NEAR:])
    starts = jnp.stack([lax.axis_index(PLANE) * segments, lax.axis_index(LINE) * segments])
    sums, _, _ = pl.pallas_call(
        lambda *refs: sums_kernel(vecs, segments, *refs),
        out_shape=(
            jax.ShapeDtypeStruct((peers, packed, 2 * segments), jnp.bfloat16),
            jax.ShapeDtypeStruct(near.shape, near.dtype),
            jax.ShapeDtypeStruct(far.shape, far.dtype),
        ),
        in_specs=[SMEM, VMEM, VMEM, VMEM],
        out_specs=(VMEM, VMEM, VMEM),
        input_output_aliases={1: 1, 2: 2},
        compiler_params=grant(16),
        name="sums",
    )(starts, near, far, right)
    parts = lax.all_to_all(sums, PLANE, 0, 0, tiled=True)
    return pl.pallas_call(
        finish_kernel,
        out_shape=jax.ShapeDtypeStruct((vecs, segments), jnp.float32),
        in_specs=[VMEM],
        out_specs=VMEM,
        compiler_params=grant(2),
        name="finish",
    )(parts)


def solution(mesh):
    torus = Mesh(mesh.devices.reshape(4, 8, 2, 4, 2), AXES)
    return jax.shard_map(
        shards,
        mesh=torus,
        in_specs=(P(None, None, AXES), P(), P(None, AXES)),
        out_specs=P(None, AXES),
        check_vma=False,
    )
```

```python
import math

import jax
import jax.numpy as jnp
from jax import lax
from jax.experimental import pallas as pl
from jax.experimental.pallas import tpu as pltpu
from jax.sharding import Mesh
from jax.sharding import PartitionSpec as P

SHARP = 3.5
AXES = ("y", "zl", "zh", "x", "core")
PLANE = ("y", "x")
LINE = ("zh", "zl", "core")
LANES = 1024
PART = 64
NEAR = 1024
SMEM = pl.BlockSpec(memory_space=pltpu.SMEM)
VMEM = pl.BlockSpec(memory_space=pltpu.VMEM)
HBM = pl.BlockSpec(memory_space=pltpu.HBM)


def grant(mib):
    return pltpu.CompilerParams(vmem_limit_bytes=mib << 20)


def prepare_kernel(
    weights_hbm, embeddings_hbm, vectors_hbm, rows_hbm, item_hbm,
    weights_ref, embeddings_ref, vectors_ref, row_ref, item_ref, in_sems, out_sems, item_sem
):
    scales, segments, dim = embeddings_ref.shape
    vecs, peers = vectors_ref.shape[0], rows_hbm.shape[0]
    count = segments // PART
    loads = [
        pltpu.make_async_copy(weights_hbm, weights_ref, in_sems.at[0]),
        pltpu.make_async_copy(vectors_hbm, vectors_ref, in_sems.at[1]),
    ] + [
        pltpu.make_async_copy(
            embeddings_hbm.at[:, part * PART : (part + 1) * PART],
            embeddings_ref.at[:, part * PART : (part + 1) * PART],
            in_sems.at[2 + part],
        )
        for part in range(count)
    ]
    for load in loads[2:] + loads[:2]:
        load.start()
    rest = LANES - scales * dim
    row_ref[:, scales * dim :] = jnp.zeros((segments, rest), jnp.bfloat16)
    loads[0].wait()
    stores = []
    for part in range(count):
        loads[2 + part].wait()
        span = slice(part * PART, (part + 1) * PART)
        units, weighted = [], []
        for scale in range(scales):
            values = embeddings_ref[scale, span, :].astype(jnp.float32)
            norm = jnp.sum(values * values, axis=1, keepdims=True) + 1e-06
            unit = (values * lax.rsqrt(norm)).astype(jnp.bfloat16).astype(jnp.float32)
            units.append(unit)
            weighted.append(weights_ref[0, scale] * unit)
        row_ref[span, : scales * dim] = jnp.concatenate(weighted, axis=1).astype(jnp.bfloat16)
        for peer in range(peers):
            store = pltpu.make_async_copy(
                row_ref.at[span], rows_hbm.at[peer, span], out_sems.at[part, peer]
            )
            store.start()
            stores.append(store)
        item_ref[span, : scales * dim] = jnp.concatenate(units, axis=1).astype(jnp.bfloat16)
    loads[1].wait()
    vectors = vectors_ref[...].astype(jnp.float32)
    top = jnp.max(jnp.abs(vectors), axis=1, keepdims=True)
    power = jnp.ceil(jnp.log2(jnp.maximum(top, 2.0**-120)))
    scaled = vectors * jnp.exp2(-power)
    powers = jnp.broadcast_to(power, (vecs, segments))
    extra = jnp.concatenate([scaled, powers], axis=0).T
    if rest > 2 * vecs:
        tail = jnp.zeros((segments, rest - 2 * vecs), jnp.float32)
        extra = jnp.concatenate([extra, tail], axis=1)
    item_ref[:, scales * dim :] = extra.astype(jnp.bfloat16)
    keep = pltpu.make_async_copy(item_ref, item_hbm, item_sem)
    keep.start()
    for store in stores:
        store.wait()
    keep.wait()


def sums_kernel(vecs, width, starts_ref, near_ref, far_ref, tail_ref, out_ref, total_ref):
    tail = tail_ref[...].astype(jnp.float32)
    count, near = tail_ref.shape[0], near_ref.shape[1]
    vectors = tail[:, :vecs] * jnp.exp2(tail[:, vecs : 2 * vecs])
    ones = jnp.ones((count, 1), jnp.float32)
    blank = jnp.zeros((count, 127 - vecs), jnp.float32)
    right = jnp.concatenate([vectors, ones, blank], axis=1).astype(jnp.bfloat16)

    def product(low, high):
        total = jnp.dot(low, right[:near], preferred_element_type=jnp.float32)
        return total + jnp.dot(high, right[near:], preferred_element_type=jnp.float32)

    def without_diagonal(part, start):
        row_place = lax.broadcasted_iota(jnp.int32, part.shape, 0)
        column_place = lax.broadcasted_iota(jnp.int32, part.shape, 1) + (start - starts_ref[1])
        kept = jnp.where(row_place == column_place, 0.0, part.astype(jnp.float32))
        return kept.astype(jnp.bfloat16)

    own = pl.ds(pl.multiple_of(starts_ref[0], width), width)
    own_product = product(
        without_diagonal(near_ref[own, :], 0), without_diagonal(far_ref[own, :], near)
    )
    total_ref[...] = product(near_ref[...], far_ref[...])
    total_ref[own, :] = own_product
    sums = total_ref[...].T[: vecs + 1].astype(jnp.bfloat16)
    half = vecs // 2
    for peer in range(out_ref.shape[0]):
        part = sums[:, peer * width : (peer + 1) * width]
        out_ref[peer, :half, :width] = part[:half]
        out_ref[peer, :half, width:] = part[half:vecs]
        out_ref[peer, half : half + 1, :width] = part[vecs:]
        out_ref[peer, half : half + 1, width:] = part[vecs:]


def finish_kernel(parts_ref, out_ref):
    half, width = out_ref.shape[0] // 2, out_ref.shape[1]
    total = jnp.sum(parts_ref[...].astype(jnp.float32), axis=0)
    product = total[:half] / total[half : half + 1]
    out_ref[:half] = product[:, :width]
    out_ref[half:] = product[:, width:]


def shards(embeddings, scale_weights, vectors):
    scales, dim, segments = embeddings.shape
    vecs = vectors.shape[0]
    peers = lax.axis_size(PLANE)
    packed = vecs // 2 + 8
    sharpness = SHARP * math.sqrt(dim) * math.log2(math.e)
    row_copies, item = pl.pallas_call(
        prepare_kernel,
        out_shape=(
            jax.ShapeDtypeStruct((peers, segments, LANES), jnp.bfloat16),
            jax.ShapeDtypeStruct((segments, LANES), jnp.bfloat16),
        ),
        in_specs=[HBM, HBM, HBM],
        out_specs=(HBM, HBM),
        scratch_shapes=[
            pltpu.SMEM((1, scales), jnp.float32),
            pltpu.VMEM((scales, segments, dim), jnp.bfloat16),
            pltpu.VMEM((vecs, segments), jnp.bfloat16),
            pltpu.VMEM((segments, LANES), jnp.bfloat16),
            pltpu.VMEM((segments, LANES), jnp.bfloat16),
            pltpu.SemaphoreType.DMA((2 + segments // PART,)),
            pltpu.SemaphoreType.DMA((segments // PART, peers)),
            pltpu.SemaphoreType.DMA(()),
        ],
        compiler_params=grant(60),
        name="prepare",
    )(scale_weights[None], jnp.swapaxes(embeddings, 1, 2), vectors)
    rows = lax.all_to_all(row_copies, PLANE, 0, 0, tiled=True)
    item = item.astype(jnp.float16).reshape(segments // 8, 8, LANES)
    columns = lax.all_gather(item, LINE, axis=0, tiled=True)
    rows, columns = lax.optimization_barrier((rows, columns))
    columns = columns.reshape(-1, LANES)
    row_count = peers * segments
    rows = rows.reshape(row_count, LANES)

    def affinity_to(part):
        cosine = lax.dot_general(
            rows,
            part.astype(jnp.bfloat16),
            (((1,), (1,)), ((), ())),
            preferred_element_type=jnp.float32,
        )
        return jnp.exp2(cosine * sharpness).astype(jnp.bfloat16)

    near = affinity_to(columns[:NEAR])
    near, late = lax.optimization_barrier((near, columns))
    far = affinity_to(late[NEAR:])
    starts = jnp.stack([lax.axis_index(PLANE) * segments, lax.axis_index(LINE) * segments])
    sums = pl.pallas_call(
        lambda *refs: sums_kernel(vecs, segments, *refs),
        out_shape=jax.ShapeDtypeStruct((peers, packed, 2 * segments), jnp.bfloat16),
        in_specs=[SMEM, VMEM, VMEM, VMEM],
        out_specs=VMEM,
        scratch_shapes=[pltpu.VMEM((row_count, 128), jnp.float32)],
        compiler_params=grant(16),
        name="sums",
    )(starts, near, far, columns[:, scales * dim :].astype(jnp.bfloat16))
    parts = lax.all_to_all(sums, PLANE, 0, 0, tiled=True)
    return pl.pallas_call(
        finish_kernel,
        out_shape=jax.ShapeDtypeStruct((vecs, segments), jnp.float32),
        in_specs=[VMEM],
        out_specs=VMEM,
        compiler_params=grant(2),
        name="finish",
    )(parts)


def solution(mesh):
    torus = Mesh(mesh.devices.reshape(4, 8, 2, 4, 2), AXES)
    return jax.shard_map(
        shards,
        mesh=torus,
        in_specs=(P(None, None, AXES), P(), P(None, AXES)),
        out_specs=P(None, AXES),
        check_vma=False,
    )
```

```python
import math

import jax
import jax.numpy as jnp
from jax import lax
from jax.experimental import pallas as pl
from jax.experimental.pallas import tpu as pltpu
from jax.sharding import Mesh
from jax.sharding import PartitionSpec as P

SHARP = 3.5
AXES = ("y", "zl", "zh", "x", "core")
PLANE = ("y", "x")
LINE = ("zh", "zl", "core")
LANES = 1024
PART = 64
NEAR = 1024
SMEM = pl.BlockSpec(memory_space=pltpu.SMEM)
VMEM = pl.BlockSpec(memory_space=pltpu.VMEM)
HBM = pl.BlockSpec(memory_space=pltpu.HBM)


def grant(mib):
    return pltpu.CompilerParams(vmem_limit_bytes=mib << 20)


def prepare_kernel(
    weights_hbm, embeddings_hbm, vectors_hbm, rows_hbm, item_hbm,
    weights_ref, embeddings_ref, vectors_ref, row_ref, item_ref, in_sems, out_sems, item_sem
):
    scales, segments, dim = embeddings_ref.shape
    vecs, peers = vectors_ref.shape[0], rows_hbm.shape[0]
    count = segments // PART
    loads = [
        pltpu.make_async_copy(weights_hbm, weights_ref, in_sems.at[0]),
        pltpu.make_async_copy(vectors_hbm, vectors_ref, in_sems.at[1]),
    ] + [
        pltpu.make_async_copy(
            embeddings_hbm.at[:, part * PART : (part + 1) * PART],
            embeddings_ref.at[:, part * PART : (part + 1) * PART],
            in_sems.at[2 + part],
        )
        for part in range(count)
    ]
    for load in loads[2:] + loads[:2]:
        load.start()
    rest = LANES - scales * dim
    row_ref[:, scales * dim :] = jnp.zeros((segments, rest), jnp.bfloat16)
    loads[0].wait()
    stores = []
    for part in range(count):
        loads[2 + part].wait()
        span = slice(part * PART, (part + 1) * PART)
        units, weighted = [], []
        for scale in range(scales):
            values = embeddings_ref[scale, span, :].astype(jnp.float32)
            norm = jnp.sum(values * values, axis=1, keepdims=True) + 1e-06
            unit = (values * lax.rsqrt(norm)).astype(jnp.bfloat16).astype(jnp.float32)
            units.append(unit)
            weighted.append(weights_ref[0, scale] * unit)
        row_ref[span, : scales * dim] = jnp.concatenate(weighted, axis=1).astype(jnp.bfloat16)
        for peer in range(peers):
            store = pltpu.make_async_copy(
                row_ref.at[span], rows_hbm.at[peer, span], out_sems.at[part, peer]
            )
            store.start()
            stores.append(store)
        item_ref[span, : scales * dim] = jnp.concatenate(units, axis=1).astype(jnp.bfloat16)
    loads[1].wait()
    vectors = vectors_ref[...].astype(jnp.float32)
    top = jnp.max(jnp.abs(vectors), axis=1, keepdims=True)
    power = jnp.ceil(jnp.log2(jnp.maximum(top, 2.0**-120)))
    scaled = vectors * jnp.exp2(-power)
    powers = jnp.broadcast_to(power, (vecs, segments))
    extra = jnp.concatenate([scaled, powers], axis=0).T
    if rest > 2 * vecs:
        tail = jnp.zeros((segments, rest - 2 * vecs), jnp.float32)
        extra = jnp.concatenate([extra, tail], axis=1)
    item_ref[:, scales * dim :] = extra.astype(jnp.bfloat16)
    keep = pltpu.make_async_copy(item_ref, item_hbm, item_sem)
    keep.start()
    for store in stores:
        store.wait()
    keep.wait()


def sums_kernel(vecs, width, starts_ref, near_ref, far_ref, tail_ref, out_ref, total_ref):
    tail = tail_ref[...].astype(jnp.float32)
    count, near = tail_ref.shape[0], near_ref.shape[1]
    vectors = tail[:, :vecs] * jnp.exp2(tail[:, vecs : 2 * vecs])
    ones = jnp.ones((count, 1), jnp.float32)
    blank = jnp.zeros((count, 127 - vecs), jnp.float32)
    right = jnp.concatenate([vectors, ones, blank], axis=1).astype(jnp.bfloat16)

    def product(low, high):
        total = jnp.dot(low, right[:near], preferred_element_type=jnp.float32)
        return total + jnp.dot(high, right[near:], preferred_element_type=jnp.float32)

    def without_diagonal(part, start):
        row_place = lax.broadcasted_iota(jnp.int32, part.shape, 0)
        column_place = lax.broadcasted_iota(jnp.int32, part.shape, 1) + (start - starts_ref[1])
        kept = jnp.where(row_place == column_place, 0.0, part.astype(jnp.float32))
        return kept.astype(jnp.bfloat16)

    own = pl.ds(pl.multiple_of(starts_ref[0], width), width)
    own_product = product(
        without_diagonal(near_ref[own, :], 0), without_diagonal(far_ref[own, :], near)
    )
    total_ref[...] = product(near_ref[...], far_ref[...])
    total_ref[own, :] = own_product
    sums = total_ref[...].T[: vecs + 1]
    half = vecs // 2
    for peer in range(out_ref.shape[0]):
        part = sums[:, peer * width : (peer + 1) * width]
        out_ref[peer, :half, :width] = part[:half]
        out_ref[peer, :half, width:] = part[half:vecs]
        out_ref[peer, half : half + 1, :width] = part[vecs:]
        out_ref[peer, half : half + 1, width:] = part[vecs:]


def finish_kernel(parts_ref, out_ref):
    half, width = out_ref.shape[0] // 2, out_ref.shape[1]
    total = jnp.sum(parts_ref[...], axis=0)
    product = total[:half] / total[half : half + 1]
    out_ref[:half] = product[:, :width]
    out_ref[half:] = product[:, width:]


def shards(embeddings, scale_weights, vectors):
    scales, dim, segments = embeddings.shape
    vecs = vectors.shape[0]
    peers = lax.axis_size(PLANE)
    packed = vecs // 2 + 8
    sharpness = SHARP * math.sqrt(dim) * math.log2(math.e)
    row_copies, item = pl.pallas_call(
        prepare_kernel,
        out_shape=(
            jax.ShapeDtypeStruct((peers, segments, LANES), jnp.bfloat16),
            jax.ShapeDtypeStruct((segments, LANES), jnp.bfloat16),
        ),
        in_specs=[HBM, HBM, HBM],
        out_specs=(HBM, HBM),
        scratch_shapes=[
            pltpu.SMEM((1, scales), jnp.float32),
            pltpu.VMEM((scales, segments, dim), jnp.bfloat16),
            pltpu.VMEM((vecs, segments), jnp.bfloat16),
            pltpu.VMEM((segments, LANES), jnp.bfloat16),
            pltpu.VMEM((segments, LANES), jnp.bfloat16),
            pltpu.SemaphoreType.DMA((2 + segments // PART,)),
            pltpu.SemaphoreType.DMA((segments // PART, peers)),
            pltpu.SemaphoreType.DMA(()),
        ],
        compiler_params=grant(60),
        name="prepare",
    )(scale_weights[None], jnp.swapaxes(embeddings, 1, 2), vectors)
    rows = lax.all_to_all(row_copies, PLANE, 0, 0, tiled=True)
    item = item.astype(jnp.float16).reshape(segments // 8, 8, LANES)
    columns = lax.all_gather(item, LINE, axis=0, tiled=True)
    rows, columns = lax.optimization_barrier((rows, columns))
    columns = columns.reshape(-1, LANES)
    row_count = peers * segments
    rows = rows.reshape(row_count, LANES)

    def affinity_to(part):
        cosine = lax.dot_general(
            rows,
            part.astype(jnp.bfloat16),
            (((1,), (1,)), ((), ())),
            preferred_element_type=jnp.float32,
        )
        return jnp.exp2(cosine * sharpness).astype(jnp.bfloat16)

    near = affinity_to(columns[:NEAR])
    near, late = lax.optimization_barrier((near, columns))
    far = affinity_to(late[NEAR:])
    starts = jnp.stack([lax.axis_index(PLANE) * segments, lax.axis_index(LINE) * segments])
    sums = pl.pallas_call(
        lambda *refs: sums_kernel(vecs, segments, *refs),
        out_shape=jax.ShapeDtypeStruct((peers, packed, 2 * segments), jnp.float32),
        in_specs=[SMEM, VMEM, VMEM, VMEM],
        out_specs=VMEM,
        scratch_shapes=[pltpu.VMEM((row_count, 128), jnp.float32)],
        compiler_params=grant(16),
        name="sums",
    )(starts, near, far, columns[:, scales * dim :].astype(jnp.bfloat16))
    parts = lax.all_to_all(sums, PLANE, 0, 0, tiled=True)
    return pl.pallas_call(
        finish_kernel,
        out_shape=jax.ShapeDtypeStruct((vecs, segments), jnp.float32),
        in_specs=[VMEM],
        out_specs=VMEM,
        compiler_params=grant(2),
        name="finish",
    )(parts)


def solution(mesh):
    torus = Mesh(mesh.devices.reshape(4, 8, 2, 4, 2), AXES)
    return jax.shard_map(
        shards,
        mesh=torus,
        in_specs=(P(None, None, AXES), P(), P(None, AXES)),
        out_specs=P(None, AXES),
        check_vma=False,
    )
```

```python
import math

import jax
import jax.numpy as jnp
from jax import lax
from jax.experimental import pallas as pl
from jax.experimental.pallas import tpu as pltpu
from jax.sharding import Mesh
from jax.sharding import PartitionSpec as P

SHARP = 3.5
AXES = ("y", "zl", "zh", "x", "core")
PLANE = ("y", "x")
LINE = ("zh", "zl", "core")
LANES = 1024
PART = 64
NEAR = 1024
SMEM = pl.BlockSpec(memory_space=pltpu.SMEM)
VMEM = pl.BlockSpec(memory_space=pltpu.VMEM)
HBM = pl.BlockSpec(memory_space=pltpu.HBM)


def grant(mib):
    return pltpu.CompilerParams(vmem_limit_bytes=mib << 20)


def prepare_kernel(
    weights_hbm, embeddings_hbm, vectors_hbm, rows_hbm, item_hbm,
    weights_ref, embeddings_ref, vectors_ref, row_ref, item_ref, in_sems, out_sems, item_sem
):
    scales, segments, dim = embeddings_ref.shape
    vecs, peers = vectors_ref.shape[0], rows_hbm.shape[0]
    count = segments // PART
    loads = [
        pltpu.make_async_copy(weights_hbm, weights_ref, in_sems.at[0]),
        pltpu.make_async_copy(vectors_hbm, vectors_ref, in_sems.at[1]),
    ] + [
        pltpu.make_async_copy(
            embeddings_hbm.at[:, part * PART : (part + 1) * PART],
            embeddings_ref.at[:, part * PART : (part + 1) * PART],
            in_sems.at[2 + part],
        )
        for part in range(count)
    ]
    for load in loads[2:] + loads[:2]:
        load.start()
    rest = LANES - scales * dim
    row_ref[:, scales * dim :] = jnp.zeros((segments, rest), jnp.bfloat16)
    loads[0].wait()
    stores = []
    for part in range(count):
        loads[2 + part].wait()
        span = slice(part * PART, (part + 1) * PART)
        units, weighted = [], []
        for scale in range(scales):
            values = embeddings_ref[scale, span, :].astype(jnp.float32)
            norm = jnp.sum(values * values, axis=1, keepdims=True) + 1e-06
            unit = (values * lax.rsqrt(norm)).astype(jnp.bfloat16).astype(jnp.float32)
            units.append(unit)
            weighted.append(weights_ref[0, scale] * unit)
        row_ref[span, : scales * dim] = jnp.concatenate(weighted, axis=1).astype(jnp.bfloat16)
        for peer in range(peers):
            store = pltpu.make_async_copy(
                row_ref.at[span], rows_hbm.at[peer, span], out_sems.at[part, peer]
            )
            store.start()
            stores.append(store)
        item_ref[span, : scales * dim] = jnp.concatenate(units, axis=1).astype(jnp.bfloat16)
    loads[1].wait()
    vectors = vectors_ref[...].astype(jnp.float32)
    top = jnp.max(jnp.abs(vectors), axis=1, keepdims=True)
    power = jnp.ceil(jnp.log2(jnp.maximum(top, 2.0**-120)))
    scaled = vectors * jnp.exp2(-power)
    powers = jnp.broadcast_to(power, (vecs, segments))
    extra = jnp.concatenate([scaled, powers], axis=0).T
    if rest > 2 * vecs:
        tail = jnp.zeros((segments, rest - 2 * vecs), jnp.float32)
        extra = jnp.concatenate([extra, tail], axis=1)
    item_ref[:, scales * dim :] = extra.astype(jnp.bfloat16)
    keep = pltpu.make_async_copy(item_ref, item_hbm, item_sem)
    keep.start()
    for store in stores:
        store.wait()
    keep.wait()


def sums_kernel(vecs, width, starts_ref, near_ref, far_ref, tail_ref, out_ref):
    tail = tail_ref[...].astype(jnp.float32)
    count, near = tail_ref.shape[0], near_ref.shape[1]
    vectors = tail[:, :vecs] * jnp.exp2(tail[:, vecs : 2 * vecs])
    ones = jnp.ones((count, 1), jnp.float32)
    blank = jnp.zeros((count, 127 - vecs), jnp.float32)
    right = jnp.concatenate([vectors, ones, blank], axis=1).astype(jnp.bfloat16)

    def product(low, high):
        total = jnp.dot(low, right[:near], preferred_element_type=jnp.float32)
        return total + jnp.dot(high, right[near:], preferred_element_type=jnp.float32)

    def without_diagonal(part, start):
        row_place = lax.broadcasted_iota(jnp.int32, part.shape, 0)
        column_place = lax.broadcasted_iota(jnp.int32, part.shape, 1) + (start - starts_ref[1])
        kept = jnp.where(row_place == column_place, 0.0, part.astype(jnp.float32))
        return kept.astype(jnp.bfloat16)

    own = pl.ds(pl.multiple_of(starts_ref[0], width), width)
    total = product(near_ref[...], far_ref[...])
    own_product = product(
        without_diagonal(near_ref[own, :], 0), without_diagonal(far_ref[own, :], near)
    )
    place = lax.broadcasted_iota(jnp.int32, (total.shape[0], 1), 0) - starts_ref[0]
    is_own = (place >= 0) & (place < width)
    copies = jnp.concatenate([own_product] * (total.shape[0] // width), axis=0)
    sums = jnp.where(is_own, copies, total).T[: vecs + 1]
    half = vecs // 2
    for peer in range(out_ref.shape[0]):
        part = sums[:, peer * width : (peer + 1) * width]
        out_ref[peer, :half, :width] = part[:half]
        out_ref[peer, :half, width:] = part[half:vecs]
        out_ref[peer, half : half + 1, :width] = part[vecs:]
        out_ref[peer, half : half + 1, width:] = part[vecs:]


def finish_kernel(parts_ref, out_ref):
    half, width = out_ref.shape[0] // 2, out_ref.shape[1]
    total = jnp.sum(parts_ref[...], axis=0)
    product = total[:half] / total[half : half + 1]
    out_ref[:half] = product[:, :width]
    out_ref[half:] = product[:, width:]


def shards(embeddings, scale_weights, vectors):
    scales, dim, segments = embeddings.shape
    vecs = vectors.shape[0]
    peers = lax.axis_size(PLANE)
    packed = vecs // 2 + 8
    sharpness = SHARP * math.sqrt(dim) * math.log2(math.e)
    row_copies, item = pl.pallas_call(
        prepare_kernel,
        out_shape=(
            jax.ShapeDtypeStruct((peers, segments, LANES), jnp.bfloat16),
            jax.ShapeDtypeStruct((segments, LANES), jnp.bfloat16),
        ),
        in_specs=[HBM, HBM, HBM],
        out_specs=(HBM, HBM),
        scratch_shapes=[
            pltpu.SMEM((1, scales), jnp.float32),
            pltpu.VMEM((scales, segments, dim), jnp.bfloat16),
            pltpu.VMEM((vecs, segments), jnp.bfloat16),
            pltpu.VMEM((segments, LANES), jnp.bfloat16),
            pltpu.VMEM((segments, LANES), jnp.bfloat16),
            pltpu.SemaphoreType.DMA((2 + segments // PART,)),
            pltpu.SemaphoreType.DMA((segments // PART, peers)),
            pltpu.SemaphoreType.DMA(()),
        ],
        compiler_params=grant(60),
        name="prepare",
    )(scale_weights[None], jnp.swapaxes(embeddings, 1, 2), vectors)
    rows = lax.all_to_all(row_copies, PLANE, 0, 0, tiled=True)
    item = item.astype(jnp.float16).reshape(segments // 8, 8, LANES)
    columns = lax.all_gather(item, LINE, axis=0, tiled=True)
    rows, columns = lax.optimization_barrier((rows, columns))
    columns = columns.reshape(-1, LANES)
    row_count = peers * segments
    rows = rows.reshape(row_count, LANES)

    def affinity_to(part):
        cosine = lax.dot_general(
            rows,
            part.astype(jnp.bfloat16),
            (((1,), (1,)), ((), ())),
            preferred_element_type=jnp.float32,
        )
        return jnp.exp2(cosine * sharpness).astype(jnp.bfloat16)

    near = affinity_to(columns[:NEAR])
    near, late = lax.optimization_barrier((near, columns))
    far = affinity_to(late[NEAR:])
    starts = jnp.stack([lax.axis_index(PLANE) * segments, lax.axis_index(LINE) * segments])
    sums = pl.pallas_call(
        lambda *refs: sums_kernel(vecs, segments, *refs),
        out_shape=jax.ShapeDtypeStruct((peers, packed, 2 * segments), jnp.float32),
        in_specs=[SMEM, VMEM, VMEM, VMEM],
        out_specs=VMEM,
        compiler_params=grant(16),
        name="sums",
    )(starts, near, far, columns[:, scales * dim :].astype(jnp.bfloat16))
    parts = lax.all_to_all(sums, PLANE, 0, 0, tiled=True)
    return pl.pallas_call(
        finish_kernel,
        out_shape=jax.ShapeDtypeStruct((vecs, segments), jnp.float32),
        in_specs=[VMEM],
        out_specs=VMEM,
        compiler_params=grant(2),
        name="finish",
    )(parts)


def solution(mesh):
    torus = Mesh(mesh.devices.reshape(4, 8, 2, 4, 2), AXES)
    return jax.shard_map(
        shards,
        mesh=torus,
        in_specs=(P(None, None, AXES), P(), P(None, AXES)),
        out_specs=P(None, AXES),
        check_vma=False,
    )
```

```python
import math

import jax
import jax.numpy as jnp
from jax import lax
from jax.experimental import pallas as pl
from jax.experimental.pallas import tpu as pltpu
from jax.sharding import Mesh
from jax.sharding import PartitionSpec as P

SHARP = 3.5
AXES = ("y", "zl", "zh", "x", "core")
PLANE = ("y", "x")
LINE = ("zh", "zl", "core")
LANES = 1024
PART = 64
NEAR = 384
SMEM = pl.BlockSpec(memory_space=pltpu.SMEM)
VMEM = pl.BlockSpec(memory_space=pltpu.VMEM)
HBM = pl.BlockSpec(memory_space=pltpu.HBM)


def grant(mib):
    return pltpu.CompilerParams(vmem_limit_bytes=mib << 20)


def prepare_kernel(
    weights_hbm, embeddings_hbm, vectors_hbm, rows_hbm, item_hbm,
    weights_ref, embeddings_ref, vectors_ref, row_ref, item_ref, in_sems, out_sems, item_sem
):
    scales, segments, dim = embeddings_ref.shape
    vecs, peers = vectors_ref.shape[0], rows_hbm.shape[0]
    count = segments // PART
    loads = [
        pltpu.make_async_copy(weights_hbm, weights_ref, in_sems.at[0]),
        pltpu.make_async_copy(vectors_hbm, vectors_ref, in_sems.at[1]),
    ] + [
        pltpu.make_async_copy(
            embeddings_hbm.at[:, part * PART : (part + 1) * PART],
            embeddings_ref.at[:, part * PART : (part + 1) * PART],
            in_sems.at[2 + part],
        )
        for part in range(count)
    ]
    for load in loads[2:] + loads[:2]:
        load.start()
    rest = LANES - scales * dim
    row_ref[:, scales * dim :] = jnp.zeros((segments, rest), jnp.bfloat16)
    loads[0].wait()
    stores = []
    for part in range(count):
        loads[2 + part].wait()
        span = slice(part * PART, (part + 1) * PART)
        units, weighted = [], []
        for scale in range(scales):
            values = embeddings_ref[scale, span, :].astype(jnp.float32)
            norm = jnp.sum(values * values, axis=1, keepdims=True) + 1e-06
            unit = (values * lax.rsqrt(norm)).astype(jnp.bfloat16).astype(jnp.float32)
            units.append(unit)
            weighted.append(weights_ref[0, scale] * unit)
        row_ref[span, : scales * dim] = jnp.concatenate(weighted, axis=1).astype(jnp.bfloat16)
        for peer in range(peers):
            store = pltpu.make_async_copy(
                row_ref.at[span], rows_hbm.at[peer, span], out_sems.at[part, peer]
            )
            store.start()
            stores.append(store)
        item_ref[span, : scales * dim] = jnp.concatenate(units, axis=1).astype(jnp.bfloat16)
    loads[1].wait()
    vectors = vectors_ref[...].astype(jnp.float32)
    top = jnp.max(jnp.abs(vectors), axis=1, keepdims=True)
    power = jnp.ceil(jnp.log2(jnp.maximum(top, 2.0**-120)))
    scaled = vectors * jnp.exp2(-power)
    powers = jnp.broadcast_to(power, (vecs, segments))
    extra = jnp.concatenate([scaled, powers], axis=0).T
    if rest > 2 * vecs:
        tail = jnp.zeros((segments, rest - 2 * vecs), jnp.float32)
        extra = jnp.concatenate([extra, tail], axis=1)
    item_ref[:, scales * dim :] = extra.astype(jnp.bfloat16)
    keep = pltpu.make_async_copy(item_ref, item_hbm, item_sem)
    keep.start()
    for store in stores:
        store.wait()
    keep.wait()


def right_kernel(vecs, tail_ref, right_ref):
    tail = tail_ref[...].astype(jnp.float32)
    vectors = tail[:, :vecs] * jnp.exp2(tail[:, vecs : 2 * vecs])
    ones = jnp.ones((tail.shape[0], 1), jnp.float32)
    blank = jnp.zeros((tail.shape[0], 127 - vecs), jnp.float32)
    right_ref[...] = jnp.concatenate([vectors, ones, blank], axis=1).astype(jnp.bfloat16)


def sums_kernel(vecs, width, starts_ref, near_ref, far_ref, right_ref, out_ref):
    near = near_ref.shape[1]

    def product(low, high):
        total = jnp.dot(low, right_ref[:near, :], preferred_element_type=jnp.float32)
        return total + jnp.dot(high, right_ref[near:, :], preferred_element_type=jnp.float32)

    def without_diagonal(part, start):
        row_place = lax.broadcasted_iota(jnp.int32, part.shape, 0)
        column_place = lax.broadcasted_iota(jnp.int32, part.shape, 1) + (start - starts_ref[1])
        kept = jnp.where(row_place == column_place, 0.0, part.astype(jnp.float32))
        return kept.astype(jnp.bfloat16)

    own = pl.ds(pl.multiple_of(starts_ref[0], width), width)
    total = product(near_ref[...], far_ref[...])
    own_product = product(
        without_diagonal(near_ref[own, :], 0), without_diagonal(far_ref[own, :], near)
    )
    place = lax.broadcasted_iota(jnp.int32, (total.shape[0], 1), 0) - starts_ref[0]
    is_own = (place >= 0) & (place < width)
    copies = jnp.concatenate([own_product] * (total.shape[0] // width), axis=0)
    sums = jnp.where(is_own, copies, total).T[: vecs + 1]
    half = vecs // 2
    for peer in range(out_ref.shape[0]):
        part = sums[:, peer * width : (peer + 1) * width]
        out_ref[peer, :half, :width] = part[:half]
        out_ref[peer, :half, width:] = part[half:vecs]
        out_ref[peer, half : half + 1, :width] = part[vecs:]
        out_ref[peer, half : half + 1, width:] = part[vecs:]


def finish_kernel(parts_ref, out_ref):
    half, width = out_ref.shape[0] // 2, out_ref.shape[1]
    total = jnp.sum(parts_ref[...], axis=0)
    product = total[:half] / total[half : half + 1]
    out_ref[:half] = product[:, :width]
    out_ref[half:] = product[:, width:]


def shards(embeddings, scale_weights, vectors):
    scales, dim, segments = embeddings.shape
    vecs = vectors.shape[0]
    peers = lax.axis_size(PLANE)
    packed = vecs // 2 + 8
    sharpness = SHARP * math.sqrt(dim) * math.log2(math.e)
    row_copies, item = pl.pallas_call(
        prepare_kernel,
        out_shape=(
            jax.ShapeDtypeStruct((peers, segments, LANES), jnp.bfloat16),
            jax.ShapeDtypeStruct((segments, LANES), jnp.bfloat16),
        ),
        in_specs=[HBM, HBM, HBM],
        out_specs=(HBM, HBM),
        scratch_shapes=[
            pltpu.SMEM((1, scales), jnp.float32),
            pltpu.VMEM((scales, segments, dim), jnp.bfloat16),
            pltpu.VMEM((vecs, segments), jnp.bfloat16),
            pltpu.VMEM((segments, LANES), jnp.bfloat16),
            pltpu.VMEM((segments, LANES), jnp.bfloat16),
            pltpu.SemaphoreType.DMA((2 + segments // PART,)),
            pltpu.SemaphoreType.DMA((segments // PART, peers)),
            pltpu.SemaphoreType.DMA(()),
        ],
        compiler_params=grant(60),
        name="prepare",
    )(scale_weights[None], jnp.swapaxes(embeddings, 1, 2), vectors)
    rows = lax.all_to_all(row_copies, PLANE, 0, 0, tiled=True)
    item = item.astype(jnp.float16).reshape(segments // 8, 8, LANES)
    columns = lax.all_gather(item, LINE, axis=0, tiled=True)
    columns = columns.reshape(-1, LANES)
    row_count = peers * segments
    rows = rows.reshape(row_count, LANES)
    right = pl.pallas_call(
        lambda *refs: right_kernel(vecs, *refs),
        out_shape=jax.ShapeDtypeStruct((columns.shape[0], 128), jnp.bfloat16),
        in_specs=[VMEM],
        out_specs=VMEM,
        compiler_params=grant(4),
        name="right",
    )(columns[:, scales * dim :].astype(jnp.bfloat16))

    def affinity_to(part):
        cosine = lax.dot_general(
            rows,
            part.astype(jnp.bfloat16),
            (((1,), (1,)), ((), ())),
            preferred_element_type=jnp.float32,
        )
        return jnp.exp2(cosine * sharpness).astype(jnp.bfloat16)

    first = lax.optimization_barrier(columns[:NEAR].astype(jnp.bfloat16))
    near = affinity_to(first)
    near, late = lax.optimization_barrier((near, columns))
    far = affinity_to(late[NEAR:])
    starts = jnp.stack([lax.axis_index(PLANE) * segments, lax.axis_index(LINE) * segments])
    sums = pl.pallas_call(
        lambda *refs: sums_kernel(vecs, segments, *refs),
        out_shape=jax.ShapeDtypeStruct((peers, packed, 2 * segments), jnp.float32),
        in_specs=[SMEM, VMEM, VMEM, VMEM],
        out_specs=VMEM,
        compiler_params=grant(16),
        name="sums",
    )(starts, near, far, right)
    parts = lax.all_to_all(sums, PLANE, 0, 0, tiled=True)
    return pl.pallas_call(
        finish_kernel,
        out_shape=jax.ShapeDtypeStruct((vecs, segments), jnp.float32),
        in_specs=[VMEM],
        out_specs=VMEM,
        compiler_params=grant(2),
        name="finish",
    )(parts)


def solution(mesh):
    torus = Mesh(mesh.devices.reshape(4, 8, 2, 4, 2), AXES)
    return jax.shard_map(
        shards,
        mesh=torus,
        in_specs=(P(None, None, AXES), P(), P(None, AXES)),
        out_specs=P(None, AXES),
        check_vma=False,
    )
```

```python
import math

import jax
import jax.numpy as jnp
from jax import lax
from jax.experimental import pallas as pl
from jax.experimental.pallas import tpu as pltpu
from jax.sharding import Mesh
from jax.sharding import PartitionSpec as P

SHARP = 3.5
AXES = ("y", "zl", "zh", "x", "core")
PLANE = ("y", "x")
LINE = ("zh", "zl", "core")
LANES = 1024
PART = 64
NEAR = 384
SMEM = pl.BlockSpec(memory_space=pltpu.SMEM)
VMEM = pl.BlockSpec(memory_space=pltpu.VMEM)
HBM = pl.BlockSpec(memory_space=pltpu.HBM)


def grant(mib):
    return pltpu.CompilerParams(vmem_limit_bytes=mib << 20)


def prepare_kernel(
    weights_hbm, embeddings_hbm, vectors_hbm, rows_hbm, item_hbm,
    weights_ref, embeddings_ref, vectors_ref, row_ref, item_ref, in_sems, out_sems, item_sem
):
    scales, segments, dim = embeddings_ref.shape
    vecs, peers = vectors_ref.shape[0], rows_hbm.shape[0]
    count = segments // PART
    loads = [
        pltpu.make_async_copy(weights_hbm, weights_ref, in_sems.at[0]),
        pltpu.make_async_copy(vectors_hbm, vectors_ref, in_sems.at[1]),
    ] + [
        pltpu.make_async_copy(
            embeddings_hbm.at[:, part * PART : (part + 1) * PART],
            embeddings_ref.at[:, part * PART : (part + 1) * PART],
            in_sems.at[2 + part],
        )
        for part in range(count)
    ]
    for load in loads[2:] + loads[:2]:
        load.start()
    rest = LANES - scales * dim
    row_ref[:, scales * dim :] = jnp.zeros((segments, rest), jnp.bfloat16)
    loads[0].wait()
    stores = []
    for part in range(count):
        loads[2 + part].wait()
        span = slice(part * PART, (part + 1) * PART)
        units, weighted = [], []
        for scale in range(scales):
            values = embeddings_ref[scale, span, :].astype(jnp.float32)
            norm = jnp.sum(values * values, axis=1, keepdims=True) + 1e-06
            unit = (values * lax.rsqrt(norm)).astype(jnp.bfloat16).astype(jnp.float32)
            units.append(unit)
            weighted.append(weights_ref[0, scale] * unit)
        row_ref[span, : scales * dim] = jnp.concatenate(weighted, axis=1).astype(jnp.bfloat16)
        for peer in range(peers):
            store = pltpu.make_async_copy(
                row_ref.at[span], rows_hbm.at[peer, span], out_sems.at[part, peer]
            )
            store.start()
            stores.append(store)
        item_ref[span, : scales * dim] = jnp.concatenate(units, axis=1).astype(jnp.bfloat16)
    loads[1].wait()
    vectors = vectors_ref[...].astype(jnp.float32)
    top = jnp.max(jnp.abs(vectors), axis=1, keepdims=True)
    power = jnp.ceil(jnp.log2(jnp.maximum(top, 2.0**-120)))
    scaled = vectors * jnp.exp2(-power)
    powers = jnp.broadcast_to(power, (vecs, segments))
    extra = jnp.concatenate([scaled, powers], axis=0).T
    if rest > 2 * vecs:
        tail = jnp.zeros((segments, rest - 2 * vecs), jnp.float32)
        extra = jnp.concatenate([extra, tail], axis=1)
    item_ref[:, scales * dim :] = extra.astype(jnp.bfloat16)
    keep = pltpu.make_async_copy(item_ref, item_hbm, item_sem)
    keep.start()
    for store in stores:
        store.wait()
    keep.wait()


def right_kernel(vecs, tail_ref, right_ref):
    tail = tail_ref[...].astype(jnp.float32)
    vectors = tail[:, :vecs] * jnp.exp2(tail[:, vecs : 2 * vecs])
    ones = jnp.ones((tail.shape[0], 1), jnp.float32)
    blank = jnp.zeros((tail.shape[0], 127 - vecs), jnp.float32)
    right_ref[...] = jnp.concatenate([vectors, ones, blank], axis=1).astype(jnp.bfloat16)


def product_of(part_ref, right_ref, starts_ref, width, start):
    right = right_ref[start : start + part_ref.shape[1], :]
    own = pl.ds(pl.multiple_of(starts_ref[0], width), width)
    total = jnp.dot(part_ref[...], right, preferred_element_type=jnp.float32)
    strip = part_ref[own, :]
    row_place = lax.broadcasted_iota(jnp.int32, strip.shape, 0)
    column_place = lax.broadcasted_iota(jnp.int32, strip.shape, 1) + (start - starts_ref[1])
    kept = jnp.where(row_place == column_place, 0.0, strip.astype(jnp.float32))
    masked = jnp.dot(kept.astype(jnp.bfloat16), right, preferred_element_type=jnp.float32)
    place = lax.broadcasted_iota(jnp.int32, (total.shape[0], 1), 0) - starts_ref[0]
    copies = jnp.concatenate([masked] * (total.shape[0] // width), axis=0)
    return jnp.where((place >= 0) & (place < width), copies, total)


def first_kernel(width, starts_ref, near_ref, right_ref, out_ref):
    out_ref[...] = product_of(near_ref, right_ref, starts_ref, width, 0)


def sums_kernel(vecs, width, near, starts_ref, first_ref, far_ref, right_ref, out_ref):
    total = first_ref[...] + product_of(far_ref, right_ref, starts_ref, width, near)
    sums = total.T[: vecs + 1]
    half = vecs // 2
    for peer in range(out_ref.shape[0]):
        part = sums[:, peer * width : (peer + 1) * width]
        out_ref[peer, :half, :width] = part[:half]
        out_ref[peer, :half, width:] = part[half:vecs]
        out_ref[peer, half : half + 1, :width] = part[vecs:]
        out_ref[peer, half : half + 1, width:] = part[vecs:]


def finish_kernel(parts_ref, out_ref):
    half, width = out_ref.shape[0] // 2, out_ref.shape[1]
    total = jnp.sum(parts_ref[...], axis=0)
    product = total[:half] / total[half : half + 1]
    out_ref[:half] = product[:, :width]
    out_ref[half:] = product[:, width:]


def shards(embeddings, scale_weights, vectors):
    scales, dim, segments = embeddings.shape
    vecs = vectors.shape[0]
    peers = lax.axis_size(PLANE)
    packed = vecs // 2 + 8
    sharpness = SHARP * math.sqrt(dim) * math.log2(math.e)
    row_copies, item = pl.pallas_call(
        prepare_kernel,
        out_shape=(
            jax.ShapeDtypeStruct((peers, segments, LANES), jnp.bfloat16),
            jax.ShapeDtypeStruct((segments, LANES), jnp.bfloat16),
        ),
        in_specs=[HBM, HBM, HBM],
        out_specs=(HBM, HBM),
        scratch_shapes=[
            pltpu.SMEM((1, scales), jnp.float32),
            pltpu.VMEM((scales, segments, dim), jnp.bfloat16),
            pltpu.VMEM((vecs, segments), jnp.bfloat16),
            pltpu.VMEM((segments, LANES), jnp.bfloat16),
            pltpu.VMEM((segments, LANES), jnp.bfloat16),
            pltpu.SemaphoreType.DMA((2 + segments // PART,)),
            pltpu.SemaphoreType.DMA((segments // PART, peers)),
            pltpu.SemaphoreType.DMA(()),
        ],
        compiler_params=grant(60),
        name="prepare",
    )(scale_weights[None], jnp.swapaxes(embeddings, 1, 2), vectors)
    rows = lax.all_to_all(row_copies, PLANE, 0, 0, tiled=True)
    item = item.astype(jnp.float16).reshape(segments // 8, 8, LANES)
    columns = lax.all_gather(item, LINE, axis=0, tiled=True)
    columns = columns.reshape(-1, LANES)
    row_count = peers * segments
    rows = rows.reshape(row_count, LANES)
    right = pl.pallas_call(
        lambda *refs: right_kernel(vecs, *refs),
        out_shape=jax.ShapeDtypeStruct((columns.shape[0], 128), jnp.bfloat16),
        in_specs=[VMEM],
        out_specs=VMEM,
        compiler_params=grant(4),
        name="right",
    )(columns[:, scales * dim :].astype(jnp.bfloat16))

    def affinity_to(part):
        cosine = lax.dot_general(
            rows,
            part.astype(jnp.bfloat16),
            (((1,), (1,)), ((), ())),
            preferred_element_type=jnp.float32,
        )
        return jnp.exp2(cosine * sharpness).astype(jnp.bfloat16)

    first = lax.optimization_barrier(columns[:NEAR].astype(jnp.bfloat16))
    near = affinity_to(first)
    starts = jnp.stack([lax.axis_index(PLANE) * segments, lax.axis_index(LINE) * segments])
    first_sums = pl.pallas_call(
        lambda *refs: first_kernel(segments, *refs),
        out_shape=jax.ShapeDtypeStruct((row_count, 128), jnp.float32),
        in_specs=[SMEM, VMEM, VMEM],
        out_specs=VMEM,
        compiler_params=grant(8),
        name="first",
    )(starts, near, right)
    first_sums, late = lax.optimization_barrier((first_sums, columns))
    far = affinity_to(late[NEAR:])
    sums = pl.pallas_call(
        lambda *refs: sums_kernel(vecs, segments, NEAR, *refs),
        out_shape=jax.ShapeDtypeStruct((peers, packed, 2 * segments), jnp.float32),
        in_specs=[SMEM, VMEM, VMEM, VMEM],
        out_specs=VMEM,
        compiler_params=grant(16),
        name="sums",
    )(starts, first_sums, far, right)
    parts = lax.all_to_all(sums, PLANE, 0, 0, tiled=True)
    return pl.pallas_call(
        finish_kernel,
        out_shape=jax.ShapeDtypeStruct((vecs, segments), jnp.float32),
        in_specs=[VMEM],
        out_specs=VMEM,
        compiler_params=grant(2),
        name="finish",
    )(parts)


def solution(mesh):
    torus = Mesh(mesh.devices.reshape(4, 8, 2, 4, 2), AXES)
    return jax.shard_map(
        shards,
        mesh=torus,
        in_specs=(P(None, None, AXES), P(), P(None, AXES)),
        out_specs=P(None, AXES),
        check_vma=False,
    )
```

```python
import math

import jax
import jax.numpy as jnp
from jax import lax
from jax.experimental import pallas as pl
from jax.experimental.pallas import tpu as pltpu
from jax.sharding import Mesh
from jax.sharding import PartitionSpec as P

SHARP = 3.5
AXES = ("y", "zl", "zh", "x", "core")
PLANE = ("y", "x")
LINE = ("zh", "zl", "core")
LANES = 1024
PART = 64
NEAR = 448
SMEM = pl.BlockSpec(memory_space=pltpu.SMEM)
VMEM = pl.BlockSpec(memory_space=pltpu.VMEM)
HBM = pl.BlockSpec(memory_space=pltpu.HBM)


def grant(mib):
    return pltpu.CompilerParams(vmem_limit_bytes=mib << 20)


def prepare_kernel(
    weights_hbm, embeddings_hbm, vectors_hbm, rows_hbm, item_hbm,
    weights_ref, embeddings_ref, vectors_ref, row_ref, item_ref, in_sems, out_sems, item_sem
):
    scales, segments, dim = embeddings_ref.shape
    vecs, peers = vectors_ref.shape[0], rows_hbm.shape[0]
    count = segments // PART
    loads = [
        pltpu.make_async_copy(weights_hbm, weights_ref, in_sems.at[0]),
        pltpu.make_async_copy(vectors_hbm, vectors_ref, in_sems.at[1]),
    ] + [
        pltpu.make_async_copy(
            embeddings_hbm.at[:, part * PART : (part + 1) * PART],
            embeddings_ref.at[:, part * PART : (part + 1) * PART],
            in_sems.at[2 + part],
        )
        for part in range(count)
    ]
    for load in loads[2:] + loads[:2]:
        load.start()
    rest = LANES - scales * dim
    row_ref[:, scales * dim :] = jnp.zeros((segments, rest), jnp.bfloat16)
    loads[0].wait()
    stores = []
    for part in range(count):
        loads[2 + part].wait()
        span = slice(part * PART, (part + 1) * PART)
        units, weighted = [], []
        for scale in range(scales):
            values = embeddings_ref[scale, span, :].astype(jnp.float32)
            norm = jnp.sum(values * values, axis=1, keepdims=True) + 1e-06
            unit = (values * lax.rsqrt(norm)).astype(jnp.bfloat16).astype(jnp.float32)
            units.append(unit)
            weighted.append(weights_ref[0, scale] * unit)
        row_ref[span, : scales * dim] = jnp.concatenate(weighted, axis=1).astype(jnp.bfloat16)
        for peer in range(peers):
            store = pltpu.make_async_copy(
                row_ref.at[span], rows_hbm.at[peer, span], out_sems.at[part, peer]
            )
            store.start()
            stores.append(store)
        item_ref[span, : scales * dim] = jnp.concatenate(units, axis=1).astype(jnp.bfloat16)
    loads[1].wait()
    vectors = vectors_ref[...].astype(jnp.float32)
    top = jnp.max(jnp.abs(vectors), axis=1, keepdims=True)
    power = jnp.ceil(jnp.log2(jnp.maximum(top, 2.0**-120)))
    scaled = vectors * jnp.exp2(-power)
    powers = jnp.broadcast_to(power, (vecs, segments))
    extra = jnp.concatenate([scaled, powers], axis=0).T
    if rest > 2 * vecs:
        tail = jnp.zeros((segments, rest - 2 * vecs), jnp.float32)
        extra = jnp.concatenate([extra, tail], axis=1)
    item_ref[:, scales * dim :] = extra.astype(jnp.bfloat16)
    keep = pltpu.make_async_copy(item_ref, item_hbm, item_sem)
    keep.start()
    for store in stores:
        store.wait()
    keep.wait()


def right_kernel(vecs, tail_ref, right_ref):
    tail = tail_ref[...].astype(jnp.float32)
    vectors = tail[:, :vecs] * jnp.exp2(tail[:, vecs : 2 * vecs])
    ones = jnp.ones((tail.shape[0], 1), jnp.float32)
    blank = jnp.zeros((tail.shape[0], 127 - vecs), jnp.float32)
    right_ref[...] = jnp.concatenate([vectors, ones, blank], axis=1).astype(jnp.bfloat16)


def sums_kernel(vecs, width, starts_ref, near_ref, far_ref, right_ref, out_ref):
    near = near_ref.shape[1]

    def product(low, high):
        total = jnp.dot(low, right_ref[:near, :], preferred_element_type=jnp.float32)
        return total + jnp.dot(high, right_ref[near:, :], preferred_element_type=jnp.float32)

    def without_diagonal(part, start):
        row_place = lax.broadcasted_iota(jnp.int32, part.shape, 0)
        column_place = lax.broadcasted_iota(jnp.int32, part.shape, 1) + (start - starts_ref[1])
        kept = jnp.where(row_place == column_place, 0.0, part.astype(jnp.float32))
        return kept.astype(jnp.bfloat16)

    own = pl.ds(pl.multiple_of(starts_ref[0], width), width)
    total = product(near_ref[...], far_ref[...])
    own_product = product(
        without_diagonal(near_ref[own, :], 0), without_diagonal(far_ref[own, :], near)
    )
    place = lax.broadcasted_iota(jnp.int32, (total.shape[0], 1), 0) - starts_ref[0]
    is_own = (place >= 0) & (place < width)
    copies = jnp.concatenate([own_product] * (total.shape[0] // width), axis=0)
    sums = jnp.where(is_own, copies, total).T[: vecs + 1]
    half = vecs // 2
    for peer in range(out_ref.shape[0]):
        part = sums[:, peer * width : (peer + 1) * width]
        out_ref[peer, :half, :width] = part[:half]
        out_ref[peer, :half, width:] = part[half:vecs]
        out_ref[peer, half : half + 1, :width] = part[vecs:]
        out_ref[peer, half : half + 1, width:] = part[vecs:]


def finish_kernel(parts_ref, out_ref):
    half, width = out_ref.shape[0] // 2, out_ref.shape[1]
    total = jnp.sum(parts_ref[...], axis=0)
    product = total[:half] / total[half : half + 1]
    out_ref[:half] = product[:, :width]
    out_ref[half:] = product[:, width:]


def shards(embeddings, scale_weights, vectors):
    scales, dim, segments = embeddings.shape
    vecs = vectors.shape[0]
    peers = lax.axis_size(PLANE)
    packed = vecs // 2 + 8
    sharpness = SHARP * math.sqrt(dim) * math.log2(math.e)
    row_copies, item = pl.pallas_call(
        prepare_kernel,
        out_shape=(
            jax.ShapeDtypeStruct((peers, segments, LANES), jnp.bfloat16),
            jax.ShapeDtypeStruct((segments, LANES), jnp.bfloat16),
        ),
        in_specs=[HBM, HBM, HBM],
        out_specs=(HBM, HBM),
        scratch_shapes=[
            pltpu.SMEM((1, scales), jnp.float32),
            pltpu.VMEM((scales, segments, dim), jnp.bfloat16),
            pltpu.VMEM((vecs, segments), jnp.bfloat16),
            pltpu.VMEM((segments, LANES), jnp.bfloat16),
            pltpu.VMEM((segments, LANES), jnp.bfloat16),
            pltpu.SemaphoreType.DMA((2 + segments // PART,)),
            pltpu.SemaphoreType.DMA((segments // PART, peers)),
            pltpu.SemaphoreType.DMA(()),
        ],
        compiler_params=grant(60),
        name="prepare",
    )(scale_weights[None], jnp.swapaxes(embeddings, 1, 2), vectors)
    rows = lax.all_to_all(row_copies, PLANE, 0, 0, tiled=True)
    item = item.astype(jnp.float16).reshape(segments // 8, 8, LANES)
    columns = lax.all_gather(item, LINE, axis=0, tiled=True)
    columns = columns.reshape(-1, LANES)
    row_count = peers * segments
    rows = rows.reshape(row_count, LANES)
    right = pl.pallas_call(
        lambda *refs: right_kernel(vecs, *refs),
        out_shape=jax.ShapeDtypeStruct((columns.shape[0], 128), jnp.bfloat16),
        in_specs=[VMEM],
        out_specs=VMEM,
        compiler_params=grant(4),
        name="right",
    )(columns[:, scales * dim :].astype(jnp.bfloat16))

    def affinity_to(part):
        cosine = lax.dot_general(
            rows,
            part.astype(jnp.bfloat16),
            (((1,), (1,)), ((), ())),
            preferred_element_type=jnp.float32,
        )
        return jnp.exp2(cosine * sharpness).astype(jnp.bfloat16)

    first = lax.optimization_barrier(columns[:NEAR].astype(jnp.bfloat16))
    near = affinity_to(first)
    near, late = lax.optimization_barrier((near, columns))
    far = affinity_to(late[NEAR:])
    starts = jnp.stack([lax.axis_index(PLANE) * segments, lax.axis_index(LINE) * segments])
    sums = pl.pallas_call(
        lambda *refs: sums_kernel(vecs, segments, *refs),
        out_shape=jax.ShapeDtypeStruct((peers, packed, 2 * segments), jnp.float32),
        in_specs=[SMEM, VMEM, VMEM, VMEM],
        out_specs=VMEM,
        compiler_params=grant(16),
        name="sums",
    )(starts, near, far, right)
    parts = lax.all_to_all(sums, PLANE, 0, 0, tiled=True)
    return pl.pallas_call(
        finish_kernel,
        out_shape=jax.ShapeDtypeStruct((vecs, segments), jnp.float32),
        in_specs=[VMEM],
        out_specs=VMEM,
        compiler_params=grant(2),
        name="finish",
    )(parts)


def solution(mesh):
    torus = Mesh(mesh.devices.reshape(4, 8, 2, 4, 2), AXES)
    return jax.shard_map(
        shards,
        mesh=torus,
        in_specs=(P(None, None, AXES), P(), P(None, AXES)),
        out_specs=P(None, AXES),
        check_vma=False,
    )
```

```python
import math

import jax
import jax.numpy as jnp
from jax import lax
from jax.experimental import pallas as pl
from jax.experimental.pallas import tpu as pltpu
from jax.sharding import Mesh
from jax.sharding import PartitionSpec as P

SHARP = 3.5
AXES = ("y", "zl", "zh", "x", "core")
PLANE = ("y", "x")
LINE = ("zh", "zl", "core")
LANES = 1024
PART = 64
NEAR = 256
SMEM = pl.BlockSpec(memory_space=pltpu.SMEM)
VMEM = pl.BlockSpec(memory_space=pltpu.VMEM)
HBM = pl.BlockSpec(memory_space=pltpu.HBM)


def grant(mib):
    return pltpu.CompilerParams(vmem_limit_bytes=mib << 20)


def prepare_kernel(
    weights_hbm, embeddings_hbm, vectors_hbm, rows_hbm, item_hbm,
    weights_ref, embeddings_ref, vectors_ref, row_ref, item_ref, in_sems, out_sems, item_sem
):
    scales, segments, dim = embeddings_ref.shape
    vecs, peers = vectors_ref.shape[0], rows_hbm.shape[0]
    count = segments // PART
    loads = [
        pltpu.make_async_copy(weights_hbm, weights_ref, in_sems.at[0]),
        pltpu.make_async_copy(vectors_hbm, vectors_ref, in_sems.at[1]),
    ] + [
        pltpu.make_async_copy(
            embeddings_hbm.at[:, part * PART : (part + 1) * PART],
            embeddings_ref.at[:, part * PART : (part + 1) * PART],
            in_sems.at[2 + part],
        )
        for part in range(count)
    ]
    for load in loads[2:] + loads[:2]:
        load.start()
    rest = LANES - scales * dim
    row_ref[:, scales * dim :] = jnp.zeros((segments, rest), jnp.bfloat16)
    loads[0].wait()
    stores = []
    for part in range(count):
        loads[2 + part].wait()
        span = slice(part * PART, (part + 1) * PART)
        units, weighted = [], []
        for scale in range(scales):
            values = embeddings_ref[scale, span, :].astype(jnp.float32)
            norm = jnp.sum(values * values, axis=1, keepdims=True) + 1e-06
            unit = (values * lax.rsqrt(norm)).astype(jnp.bfloat16).astype(jnp.float32)
            units.append(unit)
            weighted.append(weights_ref[0, scale] * unit)
        row_ref[span, : scales * dim] = jnp.concatenate(weighted, axis=1).astype(jnp.bfloat16)
        for peer in range(peers):
            store = pltpu.make_async_copy(
                row_ref.at[span], rows_hbm.at[peer, span], out_sems.at[part, peer]
            )
            store.start()
            stores.append(store)
        item_ref[span, : scales * dim] = jnp.concatenate(units, axis=1).astype(jnp.bfloat16)
    loads[1].wait()
    vectors = vectors_ref[...].astype(jnp.float32)
    top = jnp.max(jnp.abs(vectors), axis=1, keepdims=True)
    power = jnp.ceil(jnp.log2(jnp.maximum(top, 2.0**-120)))
    scaled = vectors * jnp.exp2(-power)
    powers = jnp.broadcast_to(power, (vecs, segments))
    extra = jnp.concatenate([scaled, powers], axis=0).T
    if rest > 2 * vecs:
        tail = jnp.zeros((segments, rest - 2 * vecs), jnp.float32)
        extra = jnp.concatenate([extra, tail], axis=1)
    item_ref[:, scales * dim :] = extra.astype(jnp.bfloat16)
    keep = pltpu.make_async_copy(item_ref, item_hbm, item_sem)
    keep.start()
    for store in stores:
        store.wait()
    keep.wait()


def right_kernel(vecs, tail_ref, right_ref):
    tail = tail_ref[...].astype(jnp.float32)
    vectors = tail[:, :vecs] * jnp.exp2(tail[:, vecs : 2 * vecs])
    ones = jnp.ones((tail.shape[0], 1), jnp.float32)
    blank = jnp.zeros((tail.shape[0], 127 - vecs), jnp.float32)
    right_ref[...] = jnp.concatenate([vectors, ones, blank], axis=1).astype(jnp.bfloat16)


def sums_kernel(vecs, width, starts_ref, near_ref, far_ref, right_ref, out_ref):
    near = near_ref.shape[1]

    def product(low, high):
        total = jnp.dot(low, right_ref[:near, :], preferred_element_type=jnp.float32)
        return total + jnp.dot(high, right_ref[near:, :], preferred_element_type=jnp.float32)

    def without_diagonal(part, start):
        row_place = lax.broadcasted_iota(jnp.int32, part.shape, 0)
        column_place = lax.broadcasted_iota(jnp.int32, part.shape, 1) + (start - starts_ref[1])
        kept = jnp.where(row_place == column_place, 0.0, part.astype(jnp.float32))
        return kept.astype(jnp.bfloat16)

    own = pl.ds(pl.multiple_of(starts_ref[0], width), width)
    total = product(near_ref[...], far_ref[...])
    own_product = product(
        without_diagonal(near_ref[own, :], 0), without_diagonal(far_ref[own, :], near)
    )
    place = lax.broadcasted_iota(jnp.int32, (total.shape[0], 1), 0) - starts_ref[0]
    is_own = (place >= 0) & (place < width)
    copies = jnp.concatenate([own_product] * (total.shape[0] // width), axis=0)
    sums = jnp.where(is_own, copies, total).T[: vecs + 1]
    half = vecs // 2
    for peer in range(out_ref.shape[0]):
        part = sums[:, peer * width : (peer + 1) * width]
        out_ref[peer, :half, :width] = part[:half]
        out_ref[peer, :half, width:] = part[half:vecs]
        out_ref[peer, half : half + 1, :width] = part[vecs:]
        out_ref[peer, half : half + 1, width:] = part[vecs:]


def finish_kernel(parts_ref, out_ref):
    half, width = out_ref.shape[0] // 2, out_ref.shape[1]
    total = jnp.sum(parts_ref[...], axis=0)
    product = total[:half] / total[half : half + 1]
    out_ref[:half] = product[:, :width]
    out_ref[half:] = product[:, width:]


def shards(embeddings, scale_weights, vectors):
    scales, dim, segments = embeddings.shape
    vecs = vectors.shape[0]
    peers = lax.axis_size(PLANE)
    packed = vecs // 2 + 8
    sharpness = SHARP * math.sqrt(dim) * math.log2(math.e)
    row_copies, item = pl.pallas_call(
        prepare_kernel,
        out_shape=(
            jax.ShapeDtypeStruct((peers, segments, LANES), jnp.bfloat16),
            jax.ShapeDtypeStruct((segments, LANES), jnp.bfloat16),
        ),
        in_specs=[HBM, HBM, HBM],
        out_specs=(HBM, HBM),
        scratch_shapes=[
            pltpu.SMEM((1, scales), jnp.float32),
            pltpu.VMEM((scales, segments, dim), jnp.bfloat16),
            pltpu.VMEM((vecs, segments), jnp.bfloat16),
            pltpu.VMEM((segments, LANES), jnp.bfloat16),
            pltpu.VMEM((segments, LANES), jnp.bfloat16),
            pltpu.SemaphoreType.DMA((2 + segments // PART,)),
            pltpu.SemaphoreType.DMA((segments // PART, peers)),
            pltpu.SemaphoreType.DMA(()),
        ],
        compiler_params=grant(60),
        name="prepare",
    )(scale_weights[None], jnp.swapaxes(embeddings, 1, 2), vectors)
    rows = lax.all_to_all(row_copies, PLANE, 0, 0, tiled=True)
    item = item.astype(jnp.float16).reshape(segments // 8, 8, LANES)
    columns = lax.all_gather(item, LINE, axis=0, tiled=True)
    columns = columns.reshape(-1, LANES)
    row_count = peers * segments
    rows = rows.reshape(row_count, LANES)
    right = pl.pallas_call(
        lambda *refs: right_kernel(vecs, *refs),
        out_shape=jax.ShapeDtypeStruct((columns.shape[0], 128), jnp.bfloat16),
        in_specs=[VMEM],
        out_specs=VMEM,
        compiler_params=grant(4),
        name="right",
    )(columns[:, scales * dim :].astype(jnp.bfloat16))

    def affinity_to(part):
        cosine = lax.dot_general(
            rows,
            part.astype(jnp.bfloat16),
            (((1,), (1,)), ((), ())),
            preferred_element_type=jnp.float32,
        )
        return jnp.exp2(cosine * sharpness).astype(jnp.bfloat16)

    first = lax.optimization_barrier(columns[:NEAR].astype(jnp.bfloat16))
    near = affinity_to(first)
    near, late = lax.optimization_barrier((near, columns))
    far = affinity_to(late[NEAR:])
    starts = jnp.stack([lax.axis_index(PLANE) * segments, lax.axis_index(LINE) * segments])
    sums = pl.pallas_call(
        lambda *refs: sums_kernel(vecs, segments, *refs),
        out_shape=jax.ShapeDtypeStruct((peers, packed, 2 * segments), jnp.float32),
        in_specs=[SMEM, VMEM, VMEM, VMEM],
        out_specs=VMEM,
        compiler_params=grant(16),
        name="sums",
    )(starts, near, far, right)
    parts = lax.all_to_all(sums, PLANE, 0, 0, tiled=True)
    return pl.pallas_call(
        finish_kernel,
        out_shape=jax.ShapeDtypeStruct((vecs, segments), jnp.float32),
        in_specs=[VMEM],
        out_specs=VMEM,
        compiler_params=grant(2),
        name="finish",
    )(parts)


def solution(mesh):
    torus = Mesh(mesh.devices.reshape(4, 8, 2, 4, 2), AXES)
    return jax.shard_map(
        shards,
        mesh=torus,
        in_specs=(P(None, None, AXES), P(), P(None, AXES)),
        out_specs=P(None, AXES),
        check_vma=False,
    )
```
